32 devices in a mesh: groups: 2 (over y), space: 16 (over z, x, core).
Axes of the slice: x: 2, y: 2, z: 4, core: 2. Of those that a mesh axis runs over, the one named last changes fastest.
Arguments:
- wavefield: bfloat16 [8192, 1024], P(('groups', 'space')), parts along dimension 0, may hold values from -6 to 6
- redatum_taps: float32 [512, 65], P('groups'), parts along dimension 0, may hold values from -0.75 to 0.75
- cell_x: int32 [5, 16384], replicated, may hold values from 0 to 4095
- cell_depth: int32 [16384], replicated, may hold values from 1 to 511
- slowness: float32 [4], replicated, may hold values from 0.02 to 0.2
- illumination: float32 [32768], P('groups'), parts along dimension 0, may hold values from 0.3 to 3
- aperture: int32 [8192, 1024], P(('groups', 'space')), parts along dimension 0, may hold values 0 or 1
Outputs:
- image: float32 [32, 1024], P(('groups', 'space')), parts along dimension 0
The draws below stay inside these ranges and needn't reach their ends.
There are 2 independent parts, one for each index of `groups`. The reference program is written for one: setup_inputs(seed, part) draws one part's arguments, and reference() takes and returns one part's arrays. A program takes and returns all parts, laid end to end along the dimension named above; an argument that names none is the same for every part. Nothing has to cross between parts.
All inputs are finite; a program needn't handle non-finite values. No bound on the sum of `aperture` on one device may be relied on, other than what follows from the above.
Results may differ from the reference program's by a relative error of at most 0.0075.
Values may be sent and summed in bfloat16 or wider, within the bound.
No kernel may reach another device: no remote copies, remote signals or barrier semaphores. Data moves between devices by JAX's collectives and lax.ppermute only.
A program may use at most 64 MiB of HBM per device.

```python
import math
import jax
import jax.numpy as jnp
from jax import lax

M = 1024
NF = 256
H = 32
LEVELS = 4
TAPS = 65
BOXES = 16
FREQS = 256
N_SPACE = 16


def touch_ends(array, rng, least, largest):
    longest = array.shape.index(max(array.shape))
    spots = []
    for shift in (0, 1):
        where = [jax.random.randint(jax.random.fold_in(rng, axis), (), 0, length) for axis, length in enumerate(array.shape)]
        where[longest] = (where[longest] + shift) % array.shape[longest]
        spots.append(tuple(where))
    return array.at[spots[0]].set(least).at[spots[1]].set(largest)


def level_of(key, shape, cuts, least, high):
    loudness, own = 1.0, jax.random.fold_in(key, 6)
    for position, parts in cuts:
        steps = jnp.exp(jax.random.uniform(jax.random.fold_in(own, position), (parts,), jnp.float32, least / len(cuts), high / len(cuts)))
        loudness = loudness * jnp.repeat(steps, shape[position] // parts).reshape([-1 if axis == position else 1 for axis in range(len(shape))])
    return loudness


def normal_values(key, extent, spread, limit, pieces=(), held_as=jnp.bfloat16):
    array = jax.random.normal(key, extent, jnp.float32) * spread
    if len(pieces) > 0:
        array = level_of(key, extent, pieces, -0.22, 0.18) * array
    return jnp.clip(array, min=-limit, max=limit).astype(held_as)


def setup_inputs(seed: int = 0, part: int = 0) -> dict:
    arg_keys = jax.random.split(jax.random.key(seed), 8)
    part_keys = jax.random.split(jax.random.fold_in(arg_keys[7], part), 8)
    return {
        "wavefield": normal_values(part_keys[0], (N_SPACE * NF, M), 1.0, 6.0, ((0, 16),)),
        "redatum_taps": normal_values(part_keys[1], (FREQS, TAPS), TAPS ** -0.5, 0.75, (), jnp.float32),
        "cell_x": touch_ends(jax.random.randint(arg_keys[2], (LEVELS + 1, BOXES * M), 0, 4096), jax.random.fold_in(arg_keys[2], 1), 0, 4095).astype(jnp.int32),
        "cell_depth": touch_ends(jax.random.randint(arg_keys[3], (BOXES * M,), 1, 512), jax.random.fold_in(arg_keys[3], 1), 1, 511).astype(jnp.int32),
        "slowness": jnp.clip(jnp.exp(jax.random.uniform(arg_keys[4], (LEVELS,), jnp.float32, math.log(0.02), math.log(0.2))), 0.02, 0.2),
        "illumination": jnp.clip(jnp.exp(jax.random.uniform(part_keys[5], (BOXES * M,), jnp.float32, math.log(0.3), math.log(3.0))), 0.3, 3.0),
        "aperture": touch_ends((jax.random.randint(part_keys[6], (N_SPACE * NF, M), 0, 3) < 2).astype(jnp.int32), jax.random.fold_in(part_keys[6], 1), 0, 1),
    }


def translator(rows_x, cols_x, cols_depth, slow, width):
    across = (rows_x[:, None] - cols_x[None, :]).astype(jnp.float32)
    depth = cols_depth.astype(jnp.float32)[None, :]
    travel = jnp.sqrt(across * across + depth * depth)
    return (jnp.cos(slow * travel) / jnp.sqrt(jnp.float32(width))).astype(jnp.bfloat16)

def redatum(padded, taps, width):
    total = taps[..., 0:1] * padded[..., 0:width]
    for shift in range(1, taps.shape[-1]):
        total = total + taps[..., shift:shift + 1] * padded[..., shift:shift + width]
    return total

def reference(wavefield, redatum_taps, cell_x, cell_depth, slowness, illumination, aperture):
    blocks = N_SPACE // BOXES
    wave = wavefield.reshape(BOXES, blocks, NF, M).astype(jnp.float32)
    line = jnp.transpose(wave, (1, 2, 0, 3)).reshape(blocks, NF, BOXES * M)
    padded = jnp.pad(line, ((0, 0), (0, 0), (H, H)))
    taps = redatum_taps.reshape(blocks, NF, 2 * H + 1)
    moved = redatum(padded, taps, BOXES * M).astype(jnp.bfloat16)
    state = jnp.transpose(moved.reshape(blocks, NF, BOXES, M), (2, 0, 1, 3)).reshape(BOXES, blocks * NF, M)
    for level in range(LEVELS):
        bit = 1 << level
        outputs = []
        for box in range(BOXES):
            low = box - (box & bit)
            high = low + bit
            stacked = jnp.concatenate([state[low], state[high]], 1)
            rows_x = jnp.concatenate([cell_x[level, low * M:(low + 1) * M], cell_x[level, high * M:(high + 1) * M]])
            table = translator(rows_x, cell_x[level + 1, box * M:(box + 1) * M], cell_depth[box * M:(box + 1) * M], slowness[level], M)
            outputs.append(jnp.dot(stacked, table, preferred_element_type=jnp.float32))
        mixed = jnp.stack(outputs)
        state = mixed.astype(jnp.bfloat16) if level + 1 < LEVELS else mixed
    final = state.reshape(BOXES, blocks, NF, M)
    mask = aperture.reshape(BOXES, blocks, NF, M)
    partial_value = lax.optimization_barrier(jnp.sum(jnp.where(mask > 0, final, jnp.zeros_like(final)), 2))
    partial_value = partial_value * illumination.reshape(BOXES, 1, M) / jnp.sqrt(jnp.float32(NF * blocks))
    image = lax.optimization_barrier(jnp.sum(partial_value, 1))
    share = M // blocks
    return image.reshape(BOXES * blocks, share)
```

```python
import functools
import math

import jax
import jax.numpy as jnp
from jax import lax
from jax.experimental import pallas as pl
from jax.experimental.pallas import tpu as pltpu
from jax.sharding import PartitionSpec as P

LEVELS = 4
BOXES = 16
LANES = 128
SUBLANES = 8

POLY_A = -0.55846636
POLY_B = 0.08535978
SCALE = -73.58594804
PIECES = 16
VMEM = pl.BlockSpec(memory_space=pltpu.VMEM)
SMEM = pl.BlockSpec(memory_space=pltpu.SMEM)


def params(mib):
    return pltpu.CompilerParams(vmem_limit_bytes=mib << 20)


def cost(flops, moved, transcendentals=0):
    return pl.CostEstimate(flops=flops, bytes_accessed=moved, transcendentals=transcendentals)


def passed_along(shard, axis, by):
    devices = lax.axis_size(axis)
    pairs = [(i, i + by) for i in range(devices) if 0 <= i + by < devices]
    return lax.ppermute(shard, axis, pairs)


def partner(shard, axis, bit):
    return lax.ppermute(shard, axis, [(i, i ^ 1 << bit) for i in range(lax.axis_size(axis))])


def digits(value, count):
    parts = []
    for place in range(count - 1, 0, -1):
        base = float(256**place)
        part = jnp.floor(value * (1.0 / base)) * base
        parts.append(part)
        value = value - part
    return parts + [value]


def row_pieces(x):
    x = x - 2048.0
    high = jnp.floor(x * (1.0 / 64.0)) * 64.0
    low = x - high
    one = jnp.ones_like(x)
    return [high, high, low, low] + digits(x * x, 3) + [one, one, one]


def column_pieces(x, depth):
    x = x - 2048.0
    high = jnp.floor(x * (1.0 / 64.0)) * 64.0
    low = x - high
    one = jnp.ones_like(x)
    squares = digits(x * x + depth * depth, 3)
    return [-2 * high, -2 * low, -2 * high, -2 * low, one, one, one] + squares


def stack_rows(ref, rows):
    ref[...] = jnp.zeros_like(ref)
    for k, row in enumerate(rows):
        ref[k : k + 1, :] = row


def cosine(squared, turns):
    u = (squared * lax.rsqrt(squared)) * turns
    r = u - jnp.round(u)
    w = jnp.abs(r) - 0.25
    q = w * w
    return w * ((q + POLY_A) * q + POLY_B)


def boxes_of(level, blocks):
    box = lax.axis_index("space") // blocks
    bit = 1 << level
    upper = (box // bit) % 2
    return box, box + bit - 2 * bit * upper


def tables_kernel(level, blocks, step, cell_x, cell_depth, slowness, near, far, piece, rows_b, cols_b):
    width = near.shape[0]
    last = level + 1 == LEVELS
    box, other = boxes_of(level, blocks)
    turns = slowness[level] * (0.5 / math.pi)

    def at(which):
        return pl.ds(pl.multiple_of(which * width, width), width)

    def rows_of(which):
        stack_rows(piece, row_pieces(cell_x[level : level + 1, at(which)].astype(jnp.float32)))
        rows_b[...] = piece[...].T.astype(jnp.bfloat16)

    def columns_of(which):
        x = cell_x[level + 1 : level + 2, at(which)].astype(jnp.float32)
        depth = cell_depth[pl.ds(which, 1), :].astype(jnp.float32)
        stack_rows(piece, column_pieces(x, depth))
        cols_b[...] = piece[...].astype(jnp.bfloat16)

    for out, row_box, column_box in ((near, box, box), (far, box if last else other, other if last else box)):
        if out is near or not last:
            rows_of(row_box)
        if out is near or last:
            columns_of(column_box)

        @pl.loop(0, width // step)
        def _(i):
            rows = pl.ds(pl.multiple_of(i * step, step), step)
            squared = jnp.dot(rows_b[rows, :], cols_b[...], preferred_element_type=jnp.float32)
            out[rows, :] = cosine(squared, turns).astype(jnp.bfloat16)


def tables(level, blocks, width, cell_x, cell_depth, slowness):
    shape = jax.ShapeDtypeStruct((width, width), jnp.bfloat16)
    return pl.pallas_call(
        functools.partial(tables_kernel, level, blocks, min(width, 128)),
        out_shape=(shape, shape),
        in_specs=[VMEM, VMEM, SMEM],
        out_specs=(VMEM, VMEM),
        scratch_shapes=[
            pltpu.VMEM((PIECES, width), jnp.float32),
            pltpu.VMEM((width, PIECES), jnp.bfloat16),
            pltpu.VMEM((PIECES, width), jnp.bfloat16),
        ],
        compiler_params=params(12),
        cost_estimate=cost(24 * 2 * width * width * 80, 4 * width * width),
        name=f"tables{level}",
    )(cell_x, cell_depth, slowness)


def redatum_kernel(reach, below, wave, above, taps, out, padded, taps_t):
    count, width = wave.shape
    length = taps.shape[1]
    edge = below.shape[1]
    for f in range(0, count, LANES):
        lane = f // LANES
        for source, start in ((below, 0), (wave, edge), (above, edge + width)):
            for x in range(0, source.shape[1], LANES):
                block = source[f : f + LANES, x : x + LANES].astype(jnp.float32)
                padded[lane, start + x : start + x + LANES, :] = block.T
    taps_t[...] = taps[...].T
    tiles = LANES // SUBLANES

    @pl.loop(0, width // LANES)
    def _(block):
        base = pl.multiple_of(block * LANES, LANES)
        for lane in range(count // LANES):
            sums = [jnp.zeros((SUBLANES, LANES), jnp.float32) for _ in range(tiles)]
            for rest in range(SUBLANES):
                shifts = range(rest, length, SUBLANES)
                weights = [
                    jnp.broadcast_to(
                        taps_t[j : j + 1, lane * LANES : (lane + 1) * LANES], (SUBLANES, LANES)
                    )
                    for j in shifts
                ]
                for m in range(tiles + len(weights) - 1):
                    offset = edge - reach + rest + SUBLANES * m
                    piece = padded[lane, pl.ds(base + offset, SUBLANES), :]
                    for k, weight in enumerate(weights):
                        if 0 <= m - k < tiles:
                            sums[m - k] = sums[m - k] + weight * piece
            total = jnp.concatenate(sums, 0)
            out[lane * LANES : (lane + 1) * LANES, pl.ds(base, LANES)] = total.T.astype(out.dtype)


def redatum(below, wave, above, taps):
    count, width = wave.shape
    reach = (taps.shape[1] - 1) // 2
    long = width + 2 * below.shape[1]
    return pl.pallas_call(
        functools.partial(redatum_kernel, reach),
        out_shape=jax.ShapeDtypeStruct((count, width), jnp.bfloat16),
        in_specs=[VMEM] * 4,
        out_specs=VMEM,
        scratch_shapes=[
            pltpu.VMEM((count // LANES, long, LANES), jnp.float32),
            pltpu.VMEM((taps.shape[1], count), jnp.float32),
        ],
        compiler_params=params(8),
        cost_estimate=cost(count * width * taps.shape[1] * 100, count * width * 4),
        name="redatum",
    )(below, wave, above, taps)


def mix_kernel(mine, theirs, near, far, out):
    width = near.shape[1]
    scale = SCALE / math.sqrt(width)
    step = min(width, 256)
    for c in range(0, width, step):
        columns = slice(c, c + step)
        total = jnp.dot(mine[...], near[:, columns], preferred_element_type=jnp.float32)
        total += jnp.dot(theirs[...], far[:, columns], preferred_element_type=jnp.float32)
        out[:, columns] = (total * scale).astype(out.dtype)


def mix(mine, theirs, near, far):
    count, width = mine.shape
    return pl.pallas_call(
        mix_kernel,
        out_shape=jax.ShapeDtypeStruct((count, width), jnp.bfloat16),
        in_specs=[VMEM] * 4,
        out_specs=VMEM,
        compiler_params=params(12),
        cost_estimate=cost(4 * count * width * width, 4 * width * width),
        name="mix",
    )(mine, theirs, near, far)


def last_kernel(state, near, far, own_mask, far_mask, own, other):
    width = near.shape[1]
    scale = SCALE / math.sqrt(width)
    step = min(width, 256)
    for table, mask, out in ((far, far_mask, other), (near, own_mask, own)):
        for c in range(0, width, step):
            columns = slice(c, c + step)
            mixed = jnp.dot(state[...], table[:, columns], preferred_element_type=jnp.float32)
            kept = jnp.where(mask[:, columns].astype(jnp.float32) > 0, mixed, 0.0)
            out[:, columns] = jnp.sum(kept, 0, keepdims=True) * scale


def last(state, near, far, own_mask, far_mask):
    count, width = state.shape
    shape = jax.ShapeDtypeStruct((1, width), jnp.float32)
    return pl.pallas_call(
        last_kernel,
        out_shape=(shape, shape),
        in_specs=[VMEM] * 5,
        out_specs=(VMEM, VMEM),
        compiler_params=params(12),
        cost_estimate=cost(4 * count * width * width, 4 * width * width),
        name="last",
    )(state, near, far, own_mask, far_mask)


def on_device(wavefield, redatum_taps, cell_x, cell_depth, slowness, illumination, aperture):
    index = lax.axis_index("space")
    blocks = lax.axis_size("space") // BOXES
    block_bits = blocks.bit_length() - 1
    box = index // blocks
    block = index % blocks
    count, width = wavefield.shape
    depths = cell_depth.reshape(BOXES, width)
    below = passed_along(wavefield[:, width - LANES :], "space", blocks)
    above = passed_along(wavefield[:, :LANES], "space", -blocks)
    masks = partner((aperture > 0).astype(jnp.bfloat16), "space", LEVELS - 1 + block_bits)
    taps = redatum_taps
    if blocks > 1:
        taps = lax.dynamic_slice_in_dim(redatum_taps, block * count, count, 0)
    level_tables = [
        tables(level, blocks, width, cell_x, depths, slowness) for level in range(LEVELS)
    ]
    state = redatum(below, wavefield, above, taps)
    for level in range(LEVELS - 1):
        received = partner(state, "space", level + block_bits)
        state = mix(state, received, *level_tables[level])
    own, other = last(state, *level_tables[-1], aperture, masks)
    summed = own + partner(other, "space", LEVELS - 1 + block_bits)
    weights = lax.dynamic_slice_in_dim(illumination, box * width, width)
    image = summed * weights[None] / jnp.sqrt(jnp.float32(count * blocks))
    for level in range(block_bits):
        image = image + partner(image, "space", level)
    share = width // blocks
    return lax.dynamic_slice_in_dim(image, block * share, share, 1)


def solution(mesh):
    placed = (
        P(("groups", "space"), None),
        P("groups", None),
        P(),
        P(),
        P(),
        P("groups"),
        P(("groups", "space"), None),
    )
    return jax.shard_map(
        on_device,
        mesh=mesh,
        in_specs=placed,
        out_specs=P(("groups", "space"), None),
        check_vma=False,
    )
```

```python
import functools
import math

import jax
import jax.numpy as jnp
from jax import lax
from jax.experimental import pallas as pl
from jax.experimental.pallas import tpu as pltpu
from jax.sharding import PartitionSpec as P


LEVELS = 4
BOXES = 16
LANES = 128

POLY_A = -0.55846636
POLY_B = 0.08535978
SCALE = -73.58594804
VMEM = pl.BlockSpec(memory_space=pltpu.VMEM)
ANY = pl.BlockSpec(memory_space=pl.ANY)
SMEM = pl.BlockSpec(memory_space=pltpu.SMEM)


def params(mib):
    return pltpu.CompilerParams(vmem_limit_bytes=mib << 20)


def cost(flops, moved, transcendentals=0):
    return pl.CostEstimate(flops=flops, bytes_accessed=moved, transcendentals=transcendentals)


def passed_along(shard, axis, by):
    devices = lax.axis_size(axis)
    pairs = [(i, i + by) for i in range(devices) if 0 <= i + by < devices]
    return lax.ppermute(shard, axis, pairs)


def partner(shard, axis, bit):
    return lax.ppermute(shard, axis, [(i, i ^ 1 << bit) for i in range(lax.axis_size(axis))])


def cosine(squared):
    u = squared * lax.rsqrt(squared)
    r = u - jnp.round(u)
    w = jnp.abs(r) - 0.25
    q = w * w
    return w * ((q + POLY_A) * q + POLY_B)


def boxes_of(level, blocks):
    box = lax.axis_index("space") // blocks
    bit = 1 << level
    upper = (box // bit) % 2
    return box, box + bit - 2 * bit * upper


def tables_kernel(level, blocks, step, cell_x, cell_depth, slowness, *refs):
    near, far, rows = refs[-3:]
    width = near.shape[0]
    final = level + 1 == LEVELS
    box, other = boxes_of(level, blocks)
    turns = slowness[level] * (0.5 / math.pi)

    def place(which, of):
        at = pl.ds(pl.multiple_of(which * width, width), width)
        return cell_x[of : of + 1, at].astype(jnp.float32) * turns

    for out, row_box, column_box in (
        (near, box, box),
        (far, box if final else other, other if final else box),
    ):
        if out is near or not final:
            rows[...] = jnp.broadcast_to(place(row_box, level), (LANES, width)).T
        columns = place(column_box, level + 1)
        depth = cell_depth[pl.ds(column_box, 1), :].astype(jnp.float32) * turns
        below = depth * depth

        @pl.loop(0, width // step)
        def _(i):
            at = pl.ds(pl.multiple_of(i * step, step), step)
            for c in range(0, width, 2 * LANES):
                part = rows[at, :]
                across = jnp.concatenate([part, part], 1) - columns[:, c : c + 2 * LANES]
                squared = across * across + below[:, c : c + 2 * LANES]
                out[at, c : c + 2 * LANES] = cosine(squared).astype(jnp.bfloat16)


def tables(level, blocks, width, cell_x, cell_depth, slowness, *after):
    shape = jax.ShapeDtypeStruct((width, width), jnp.bfloat16)
    return pl.pallas_call(
        functools.partial(tables_kernel, level, blocks, min(width, 128)),
        out_shape=(shape, shape),
        in_specs=[VMEM, VMEM, SMEM] + [ANY] * len(after),
        out_specs=(VMEM, VMEM),
        scratch_shapes=[pltpu.VMEM((width, LANES), jnp.float32)],
        compiler_params=params(7),
        cost_estimate=cost(24 * 2 * width * width * 40, 4 * width * width),
    )(cell_x, cell_depth, slowness, *after)


def redatum_kernel(reach, part, below, wave, above, taps, *refs):
    out, padded = refs[-2:]
    width = wave.shape[1]
    edge = below.shape[1]
    held = slice(part * LANES, (part + 1) * LANES)
    for source, start in ((below, 0), (wave, edge), (above, edge + width)):
        for x in range(0, source.shape[1], LANES):
            block = source[held, x : x + LANES].astype(jnp.float32)
            padded[start + x : start + x + LANES, :] = block.T

    @pl.loop(0, width // LANES)
    def _(block):
        base = pl.multiple_of(block * LANES, LANES)
        total = None
        for j in range(taps.shape[0]):
            weight = jnp.broadcast_to(taps[j : j + 1, held], (LANES, LANES))
            term = weight * padded[pl.ds(base + edge - reach + j, LANES), :]
            total = term if total is None else total + term
        out[:, pl.ds(base, LANES)] = total.T.astype(out.dtype)


def redatum(part, below, wave, above, taps, *after):
    width = wave.shape[1]
    reach = (taps.shape[0] - 1) // 2
    long = width + 2 * below.shape[1]
    return pl.pallas_call(
        functools.partial(redatum_kernel, reach, part),
        out_shape=jax.ShapeDtypeStruct((LANES, width), jnp.bfloat16),
        in_specs=[VMEM] * 4 + [ANY] * len(after),
        out_specs=VMEM,
        scratch_shapes=[pltpu.VMEM((long, LANES), jnp.float32)],
        compiler_params=params(5),
        cost_estimate=cost(24 * 2 * width * width * 30, LANES * width * 4),
    )(below, wave, above, taps, *after)


def mix_kernel(mine, theirs, near, far, *refs):
    out = refs[-1]
    width = near.shape[1]
    scale = SCALE / math.sqrt(width)
    step = min(width, 256)
    for c in range(0, width, step):
        columns = slice(c, c + step)
        total = jnp.dot(mine[...], near[:, columns], preferred_element_type=jnp.float32)
        total += jnp.dot(theirs[...], far[:, columns], preferred_element_type=jnp.float32)
        out[:, columns] = (total * scale).astype(out.dtype)


def mix(mine, theirs, near, far, *after):
    count, width = mine.shape
    return pl.pallas_call(
        mix_kernel,
        out_shape=jax.ShapeDtypeStruct((count, width), jnp.bfloat16),
        in_specs=[VMEM] * 4 + [ANY] * len(after),
        out_specs=VMEM,
        compiler_params=params(7),
        cost_estimate=cost(4 * count * width * width, 4 * width * width),
        name="mix",
    )(mine, theirs, near, far, *after)


def last_kernel(part, state, near, far, own_mask, far_mask, *refs):
    own, other = refs[-2:]
    width = near.shape[1]
    scale = SCALE / math.sqrt(width)
    step = min(width, 256)
    held = slice(part * LANES, (part + 1) * LANES)
    for k, (table, mask, out) in enumerate(((far, far_mask, other), (near, own_mask, own))):
        for c in range(0, width, step):
            columns = slice(c, c + step)
            mixed = jnp.dot(state[...], table[:, columns], preferred_element_type=jnp.float32)
            kept = jnp.where(mask[held, columns].astype(jnp.float32) > 0, mixed, 0.0)
            total = jnp.sum(kept, 0, keepdims=True) * scale
            if part > 0:
                total = total + refs[1 - k][:, columns]
            out[:, columns] = total


def last(part, state, near, far, own_mask, far_mask, sums, *after):
    count, width = state.shape
    shape = jax.ShapeDtypeStruct((1, width), jnp.float32)
    return pl.pallas_call(
        functools.partial(last_kernel, part),
        out_shape=(shape, shape),
        in_specs=[VMEM] * (5 + len(sums)) + [ANY] * len(after),
        out_specs=(VMEM, VMEM),
        compiler_params=params(8),
        cost_estimate=cost(4 * count * width * width, 4 * width * width),
    )(state, near, far, own_mask, far_mask, *sums, *after)


def on_device(wavefield, redatum_taps, cell_x, cell_depth, slowness, illumination, aperture):
    index = lax.axis_index("space")
    blocks = lax.axis_size("space") // BOXES
    block_bits = blocks.bit_length() - 1
    box = index // blocks
    block = index % blocks
    count, width = wavefield.shape
    depths = cell_depth.reshape(BOXES, width)
    below = passed_along(wavefield[:, width - LANES :], "space", blocks)
    above = passed_along(wavefield[:, :LANES], "space", -blocks)
    mask = (aperture > 0).astype(jnp.bfloat16)
    masks = partner(mask, "space", LEVELS - 1 + block_bits)
    taps = redatum_taps
    if blocks > 1:
        taps = lax.dynamic_slice_in_dim(redatum_taps, block * count, count, 0)
    taps = taps.T
    parts = range(count // LANES)

    def exchange(states, level):
        return [partner(state, "space", level + block_bits) for state in states]

    shared = (blocks, width, cell_x, depths, slowness)
    table = tables(0, *shared, mask)
    states, ahead = [], table[0]
    for part in parts:
        states.append(redatum(part, below, wavefield, above, taps, ahead))
        ahead = states[-1]
    for level in range(LEVELS - 1):
        received = exchange(states, level)
        for part in parts:
            states[part] = mix(states[part], received[part], *table, ahead)
            ahead = states[part]
            if part == 0 and level > 0:
                following = tables(level + 1, *shared, ahead)
                ahead = following[0]
        if level == 0:
            following = tables(level + 1, *shared, ahead)
            ahead = following[0]
        table = following
    sums = ()
    for part in parts:
        sums = last(part, states[part], *table, aperture, masks, sums)
    own, other = sums
    summed = own + partner(other, "space", LEVELS - 1 + block_bits)
    weights = lax.dynamic_slice_in_dim(illumination, box * width, width)
    image = summed * weights[None] / jnp.sqrt(jnp.float32(count * blocks))
    for level in range(block_bits):
        image = image + partner(image, "space", level)
    share = width // blocks
    return lax.dynamic_slice_in_dim(image, block * share, share, 1)


def solution(mesh):
    placed = (
        P(("groups", "space"), None),
        P("groups", None),
        P(),
        P(),
        P(),
        P("groups"),
        P(("groups", "space"), None),
    )
    return jax.shard_map(
        on_device,
        mesh=mesh,
        in_specs=placed,
        out_specs=P(("groups", "space"), None),
        check_vma=False,
    )
```

```python
import functools
import math

import jax
import jax.numpy as jnp
from jax import lax
from jax.experimental import pallas as pl
from jax.experimental.pallas import tpu as pltpu
from jax.sharding import PartitionSpec as P


LEVELS = 4
BOXES = 16
LANES = 128

POLY_A = -0.55846636
POLY_B = 0.08535978
SCALE = -73.58594804
VMEM = pl.BlockSpec(memory_space=pltpu.VMEM)
ANY = pl.BlockSpec(memory_space=pl.ANY)
SMEM = pl.BlockSpec(memory_space=pltpu.SMEM)


def params(mib):
    return pltpu.CompilerParams(vmem_limit_bytes=mib << 20)


def cost(flops, moved, transcendentals=0):
    return pl.CostEstimate(flops=flops, bytes_accessed=moved, transcendentals=transcendentals)


def passed_along(shard, axis, by):
    devices = lax.axis_size(axis)
    pairs = [(i, i + by) for i in range(devices) if 0 <= i + by < devices]
    return lax.ppermute(shard, axis, pairs)


def partner(shard, axis, bit):
    return lax.ppermute(shard, axis, [(i, i ^ 1 << bit) for i in range(lax.axis_size(axis))])


def cosine(squared):
    u = squared * lax.rsqrt(squared)
    r = u - jnp.round(u)
    w = jnp.abs(r) - 0.25
    q = w * w
    return w * ((q + POLY_A) * q + POLY_B)


def boxes_of(level, blocks):
    box = lax.axis_index("space") // blocks
    bit = 1 << level
    upper = (box // bit) % 2
    return box, box + bit - 2 * bit * upper


ROW, OTHER_ROW, COLUMN, BELOW, OTHER_COLUMN, OTHER_BELOW = range(6)


def prepare_kernel(blocks, wave, aperture, cell_x, depth, slowness, *refs):
    head, tail, mask, coords, cells, depths, slow, marks, sems = refs
    width = wave.shape[1]
    tall = width // LANES
    box = boxes_of(0, blocks)[0]
    others = [boxes_of(level, blocks)[1] for level in range(LEVELS)]
    copies = [pltpu.make_async_copy(slowness, slow, sems.at[0])]
    for k, which in enumerate([box] + others):
        at = pl.ds(pl.multiple_of(which * width, width), width)
        copies.append(pltpu.make_async_copy(cell_x.at[:, at], cells.at[k], sems.at[1 + k]))
    for k, which in enumerate((box, others[-1])):
        at = pl.ds(pl.multiple_of(which * tall, tall), tall)
        copies.append(pltpu.make_async_copy(depth.at[at, :], depths.at[k], sems.at[6 + k]))
    late = [
        pltpu.make_async_copy(wave.at[:, pl.ds(0, LANES)], head, sems.at[8]),
        pltpu.make_async_copy(wave.at[:, pl.ds(width - LANES, LANES)], tail, sems.at[9]),
        pltpu.make_async_copy(aperture, marks, sems.at[10]),
    ]
    for copy in copies + late:
        copy.start()
    for copy in copies:
        copy.wait()
    coords[...] = jnp.zeros_like(coords)
    for level in range(LEVELS):
        turns = slow[level] * (0.5 / math.pi)
        base = 8 * level

        def put(kind, source, row):
            coords[base + kind : base + kind + 1, :] = (
                cells[source, row : row + 1, :].astype(jnp.float32) * turns
            )

        def put_below(kind, source):
            for k in range(tall):
                part = depths[source, k : k + 1, :].astype(jnp.float32) * turns
                coords[base + kind : base + kind + 1, k * LANES : (k + 1) * LANES] = part * part

        put(ROW, 0, level)
        put(OTHER_ROW, 1 + level, level)
        put(COLUMN, 0, level + 1)
        put_below(BELOW, 0)
        if level + 1 == LEVELS:
            put(OTHER_COLUMN, LEVELS, level + 1)
            put_below(OTHER_BELOW, 1)
    for copy in late:
        copy.wait()
    mask[...] = (marks[...] > 0).astype(jnp.float32).astype(jnp.bfloat16)


def prepare(blocks, wave, aperture, cell_x, depth, slowness):
    count, width = wave.shape
    levels = cell_x.shape[0]
    edge = jax.ShapeDtypeStruct((count, LANES), wave.dtype)
    return pl.pallas_call(
        functools.partial(prepare_kernel, blocks),
        out_shape=(
            edge,
            edge,
            jax.ShapeDtypeStruct((count, width), jnp.bfloat16),
            jax.ShapeDtypeStruct((8 * LEVELS, width), jnp.float32),
        ),
        in_specs=[ANY] * 5,
        out_specs=(VMEM,) * 4,
        scratch_shapes=[
            pltpu.VMEM((1 + LEVELS, levels, width), jnp.int32),
            pltpu.VMEM((2, width // LANES, LANES), jnp.int32),
            pltpu.SMEM((LEVELS,), jnp.float32),
            pltpu.VMEM((count, width), jnp.int32),
            pltpu.SemaphoreType.DMA((11,)),
        ],
        compiler_params=params(6),
        cost_estimate=cost(24 * 2 * width * width * 15, count * width * 8),
        name="prepare",
    )(wave, aperture, cell_x, depth, slowness)


def tables_kernel(jobs, step, coords, *refs):
    outs, rows = refs[-1 - len(jobs) : -1], refs[-1]
    width = outs[0].shape[0]
    steps = width // step

    def fill(slot, row, i):
        at = pl.ds(pl.multiple_of(i * step, step), step)
        rows[slot] = jnp.broadcast_to(coords[row : row + 1, at], (LANES, step)).T

    for (row, column, below), out in zip(jobs, outs):
        fill(0, row, 0)

        @pl.loop(0, steps)
        def _(i):
            at = pl.ds(pl.multiple_of(i * step, step), step)
            part = rows[i % 2]
            part = jnp.concatenate([part, part], 1)
            for c in range(0, width, 2 * LANES):
                columns = slice(c, c + 2 * LANES)
                across = part - coords[column : column + 1, columns]
                squared = across * across + coords[below : below + 1, columns]
                out[at, columns] = cosine(squared).astype(jnp.bfloat16)
            fill((i + 1) % 2, row, jnp.minimum(i + 1, steps - 1))


def tables(level, which, coords, *after):
    width = coords.shape[1]
    base = 8 * level
    near = (base + ROW, base + COLUMN, base + BELOW)
    far = (base + OTHER_ROW, base + COLUMN, base + BELOW)
    if level + 1 == LEVELS:
        far = (base + ROW, base + OTHER_COLUMN, base + OTHER_BELOW)
    jobs = [(near, far)[k] for k in which]
    shape = jax.ShapeDtypeStruct((width, width), jnp.bfloat16)
    step = LANES
    return pl.pallas_call(
        functools.partial(tables_kernel, jobs, step),
        out_shape=(shape,) * len(jobs),
        in_specs=[VMEM] + [ANY] * len(after),
        out_specs=(VMEM,) * len(jobs),
        scratch_shapes=[pltpu.VMEM((2, step, LANES), jnp.float32)],
        compiler_params=params(6),
        cost_estimate=cost(24 * len(jobs) * width * width * 40, 2 * len(jobs) * width * width),
    )(coords, *after)


def redatum_kernel(reach, below, wave, above, taps, *refs):
    out, padded = refs[-2:]
    count, width = wave.shape
    edge = below.shape[1]
    blocks = width // LANES
    halves = range(count // LANES)

    def held(lane):
        return slice(lane * LANES, (lane + 1) * LANES)

    def fill(source, x, start):
        for lane in halves:
            block = source[held(lane), pl.ds(x, LANES)].astype(jnp.float32)
            padded[lane, pl.ds(start, LANES), :] = block.T

    fill(below, 0, 0)
    fill(above, 0, edge + width)
    for k in range(min(2, blocks)):
        fill(wave, k * LANES, edge + k * LANES)

    @pl.loop(0, blocks)
    def _(block):
        base = pl.multiple_of(block * LANES, LANES)
        for lane in halves:
            total = None
            for j in range(taps.shape[0]):
                weight = jnp.broadcast_to(taps[j : j + 1, held(lane)], (LANES, LANES))
                term = weight * padded[lane, pl.ds(base + edge - reach + j, LANES), :]
                total = term if total is None else total + term
            out[held(lane), pl.ds(base, LANES)] = total.T.astype(out.dtype)
        ahead = pl.multiple_of(jnp.minimum(block + 2, blocks - 1) * LANES, LANES)
        fill(wave, ahead, edge + ahead)


def redatum(below, wave, above, taps, *after):
    count, width = wave.shape
    reach = (taps.shape[0] - 1) // 2
    long = width + 2 * below.shape[1]
    return pl.pallas_call(
        functools.partial(redatum_kernel, reach),
        out_shape=jax.ShapeDtypeStruct((count, width), jnp.bfloat16),
        in_specs=[VMEM] * 4 + [ANY] * len(after),
        out_specs=VMEM,
        scratch_shapes=[pltpu.VMEM((count // LANES, long, LANES), jnp.float32)],
        compiler_params=params(6),
        cost_estimate=cost(24 * 2 * width * width * 60, count * width * 4),
        name="redatum",
    )(below, wave, above, taps, *after)


def mix_kernel(held, mine, theirs, near, far, *refs):
    out = refs[-1]
    width = near.shape[1]
    scale = SCALE / math.sqrt(width)
    step = min(width, 256)
    for c in range(0, width, step):
        columns = slice(c, c + step)
        total = jnp.dot(mine[held, :], near[:, columns], preferred_element_type=jnp.float32)
        total += jnp.dot(theirs[held, :], far[:, columns], preferred_element_type=jnp.float32)
        out[:, columns] = (total * scale).astype(out.dtype)


def mix(part, mine, theirs, near, far, *after):
    count, width = mine.shape
    held = slice(part * LANES, (part + 1) * LANES) if count > LANES else slice(0, LANES)
    return pl.pallas_call(
        functools.partial(mix_kernel, held),
        out_shape=jax.ShapeDtypeStruct((LANES, width), jnp.bfloat16),
        in_specs=[VMEM] * 4 + [ANY] * len(after),
        out_specs=VMEM,
        compiler_params=params(7),
        cost_estimate=cost(24 * width * width * 15, 4 * width * width),
        name="mix",
    )(mine, theirs, near, far, *after)


def last_kernel(part, state, near, far, own_mask, far_mask, *refs):
    own, other = refs[-2:]
    width = near.shape[1]
    scale = SCALE / math.sqrt(width)
    step = min(width, 256)
    held = slice(part * LANES, (part + 1) * LANES)
    for k, (table, mask, out) in enumerate(((far, far_mask, other), (near, own_mask, own))):
        for c in range(0, width, step):
            columns = slice(c, c + step)
            mixed = jnp.dot(state[...], table[:, columns], preferred_element_type=jnp.float32)
            kept = jnp.where(mask[held, columns].astype(jnp.float32) > 0, mixed, 0.0)
            total = jnp.sum(kept, 0, keepdims=True) * scale
            if part > 0:
                total = total + refs[1 - k][:, columns]
            out[:, columns] = total


def last(part, state, near, far, own_mask, far_mask, sums, *after):
    count, width = state.shape
    shape = jax.ShapeDtypeStruct((1, width), jnp.float32)
    return pl.pallas_call(
        functools.partial(last_kernel, part),
        out_shape=(shape, shape),
        in_specs=[VMEM] * (5 + len(sums)) + [ANY] * len(after),
        out_specs=(VMEM, VMEM),
        compiler_params=params(8),
        cost_estimate=cost(4 * count * width * width, 4 * width * width),
    )(state, near, far, own_mask, far_mask, *sums, *after)


def on_device(wavefield, redatum_taps, cell_x, cell_depth, slowness, illumination, aperture):
    index = lax.axis_index("space")
    blocks = lax.axis_size("space") // BOXES
    block_bits = blocks.bit_length() - 1
    box = index // blocks
    block = index % blocks
    count, width = wavefield.shape
    depth = cell_depth.reshape(BOXES * width // LANES, LANES)
    head, tail, mask, coords = prepare(blocks, wavefield, aperture, cell_x, depth, slowness)
    below = passed_along(tail, "space", blocks)
    above = passed_along(head, "space", -blocks)
    masks = partner(mask, "space", LEVELS - 1 + block_bits)
    taps = redatum_taps
    if blocks > 1:
        taps = lax.dynamic_slice_in_dim(redatum_taps, block * count, count, 0)
    taps = taps.T
    parts = range(count // LANES)

    (near,) = tables(0, (0,), coords)
    state = redatum(below, wavefield, above, taps, near)
    received = partner(state, "space", block_bits)
    (far,) = tables(0, (1,), coords, state)
    states = [state for _ in parts]
    theirs = [received for _ in parts]
    table, ahead = (near, far), far
    for level in range(LEVELS - 1):
        for part in parts:
            states[part] = mix(part, states[part], theirs[part], *table, ahead)
            ahead = states[part]
            if level + 2 < LEVELS:
                theirs[part] = partner(states[part], "space", level + 1 + block_bits)
            if part == (len(parts) - 1 if level == 0 else 0):
                following = tables(level + 1, (0, 1), coords, ahead)
                ahead = following[0]
        table = following
    sums = ()
    for part in parts:
        sums = last(part, states[part], *table, mask, masks, sums)
    own, other = sums
    summed = own + partner(other, "space", LEVELS - 1 + block_bits)
    weights = lax.dynamic_slice_in_dim(illumination, box * width, width)
    image = summed * weights[None] / jnp.sqrt(jnp.float32(count * blocks))
    for level in range(block_bits):
        image = image + partner(image, "space", level)
    share = width // blocks
    return lax.dynamic_slice_in_dim(image, block * share, share, 1)


def solution(mesh):
    placed = (
        P(("groups", "space"), None),
        P("groups", None),
        P(),
        P(),
        P(),
        P("groups"),
        P(("groups", "space"), None),
    )
    return jax.shard_map(
        on_device,
        mesh=mesh,
        in_specs=placed,
        out_specs=P(("groups", "space"), None),
        check_vma=False,
    )
```

```python
import functools
import math

import jax
import jax.numpy as jnp
from jax import lax
from jax.experimental import pallas as pl
from jax.experimental.pallas import tpu as pltpu
from jax.sharding import PartitionSpec as P


LEVELS = 4
BOXES = 16
LANES = 128

POLY_A = -0.55846636
POLY_B = 0.08535978
SCALE = -73.58594804
VMEM = pl.BlockSpec(memory_space=pltpu.VMEM)
GRANT = 56 << 20
ANY = pl.BlockSpec(memory_space=pl.ANY)
HBM = pl.BlockSpec(memory_space=pltpu.HBM)
SMEM = pl.BlockSpec(memory_space=pltpu.SMEM)


def params(mib):
    return pltpu.CompilerParams(vmem_limit_bytes=mib << 20)


def cost(flops, moved, transcendentals=0):
    return pl.CostEstimate(flops=flops, bytes_accessed=moved, transcendentals=transcendentals)


def passed_along(shard, axis, by):
    devices = lax.axis_size(axis)
    pairs = [(i, i + by) for i in range(devices) if 0 <= i + by < devices]
    return lax.ppermute(shard, axis, pairs)


def partner(shard, axis, bit):
    return lax.ppermute(shard, axis, [(i, i ^ 1 << bit) for i in range(lax.axis_size(axis))])


def cosine(squared):
    u = squared * lax.rsqrt(squared)
    r = u - jnp.round(u)
    w = jnp.abs(r) - 0.25
    q = w * w
    return w * ((q + POLY_A) * q + POLY_B)


def boxes_of(level, blocks):
    box = lax.axis_index("space") // blocks
    bit = 1 << level
    upper = (box // bit) % 2
    return box, box + bit - 2 * bit * upper


ROW, OTHER_ROW, COLUMN, BELOW, OTHER_COLUMN, OTHER_BELOW = range(6)


def prepare_kernel(blocks, wave, aperture, cell_x, depth, slowness, *refs):
    head, tail, mask, coords, cells, depths, slow, marks, sems = refs
    width = wave.shape[1]
    tall = width // LANES
    box = boxes_of(0, blocks)[0]
    others = [boxes_of(level, blocks)[1] for level in range(LEVELS)]
    copies = [pltpu.make_async_copy(slowness, slow, sems.at[0])]
    for k, which in enumerate([box] + others):
        at = pl.ds(pl.multiple_of(which * width, width), width)
        copies.append(pltpu.make_async_copy(cell_x.at[:, at], cells.at[k], sems.at[1 + k]))
    for k, which in enumerate((box, others[-1])):
        at = pl.ds(pl.multiple_of(which * tall, tall), tall)
        copies.append(pltpu.make_async_copy(depth.at[at, :], depths.at[k], sems.at[6 + k]))
    late = [
        pltpu.make_async_copy(wave.at[:, pl.ds(0, LANES)], head, sems.at[8]),
        pltpu.make_async_copy(wave.at[:, pl.ds(width - LANES, LANES)], tail, sems.at[9]),
        pltpu.make_async_copy(aperture, marks, sems.at[10]),
    ]
    for copy in copies + late:
        copy.start()
    for copy in copies:
        copy.wait()
    coords[...] = jnp.zeros_like(coords)
    for level in range(LEVELS):
        turns = slow[level] * (0.5 / math.pi)
        base = 8 * level

        def put(kind, source, row):
            coords[base + kind : base + kind + 1, :] = (
                cells[source, row : row + 1, :].astype(jnp.float32) * turns
            )

        def put_below(kind, source):
            for k in range(tall):
                part = depths[source, k : k + 1, :].astype(jnp.float32) * turns
                coords[base + kind : base + kind + 1, k * LANES : (k + 1) * LANES] = part * part

        put(ROW, 0, level)
        put(OTHER_ROW, 1 + level, level)
        put(COLUMN, 0, level + 1)
        put_below(BELOW, 0)
        if level + 1 == LEVELS:
            put(OTHER_COLUMN, LEVELS, level + 1)
            put_below(OTHER_BELOW, 1)
    for copy in late:
        copy.wait()
    mask[...] = (marks[...] > 0).astype(jnp.float32).astype(jnp.bfloat16)


def prepare(blocks, wave, aperture, cell_x, depth, slowness):
    count, width = wave.shape
    levels = cell_x.shape[0]
    edge = jax.ShapeDtypeStruct((count, LANES), wave.dtype)
    return pl.pallas_call(
        functools.partial(prepare_kernel, blocks),
        out_shape=(
            edge,
            edge,
            jax.ShapeDtypeStruct((count, width), jnp.bfloat16),
            jax.ShapeDtypeStruct((8 * LEVELS, width), jnp.float32),
        ),
        in_specs=[HBM] * 5,
        out_specs=(VMEM,) * 4,
        scratch_shapes=[
            pltpu.VMEM((1 + LEVELS, levels, width), jnp.int32),
            pltpu.VMEM((2, width // LANES, LANES), jnp.int32),
            pltpu.SMEM((LEVELS,), jnp.float32),
            pltpu.VMEM((count, width), jnp.int32),
            pltpu.SemaphoreType.DMA((11,)),
        ],
        compiler_params=pltpu.CompilerParams(vmem_limit_bytes=GRANT),
        cost_estimate=cost(24 * 2 * width * width * 15, count * width * 8),
        name="prepare",
    )(wave, aperture, cell_x, depth, slowness)


def tables_kernel(jobs, step, coords, *refs):
    outs, rows = refs[-1 - len(jobs) : -1], refs[-1]
    width = outs[0].shape[0]
    steps = width // step

    def fill(slot, row, i):
        at = pl.ds(pl.multiple_of(i * step, step), step)
        rows[slot] = jnp.broadcast_to(coords[row : row + 1, at], (LANES, step)).T

    for (row, column, below), out in zip(jobs, outs):
        fill(0, row, 0)

        @pl.loop(0, steps)
        def _(i):
            at = pl.ds(pl.multiple_of(i * step, step), step)
            part = rows[i % 2]
            part = jnp.concatenate([part, part], 1)
            for c in range(0, width, 2 * LANES):
                columns = slice(c, c + 2 * LANES)
                across = part - coords[column : column + 1, columns]
                squared = across * across + coords[below : below + 1, columns]
                out[at, columns] = cosine(squared).astype(jnp.bfloat16)
            fill((i + 1) % 2, row, jnp.minimum(i + 1, steps - 1))


def tables(level, which, coords, *after):
    width = coords.shape[1]
    base = 8 * level
    near = (base + ROW, base + COLUMN, base + BELOW)
    far = (base + OTHER_ROW, base + COLUMN, base + BELOW)
    if level + 1 == LEVELS:
        far = (base + ROW, base + OTHER_COLUMN, base + OTHER_BELOW)
    jobs = [(near, far)[k] for k in which]
    shape = jax.ShapeDtypeStruct((width, width), jnp.bfloat16)
    step = LANES
    return pl.pallas_call(
        functools.partial(tables_kernel, jobs, step),
        out_shape=(shape,) * len(jobs),
        in_specs=[VMEM] + [ANY] * len(after),
        out_specs=(VMEM,) * len(jobs),
        scratch_shapes=[pltpu.VMEM((2, step, LANES), jnp.float32)],
        compiler_params=params(6),
        cost_estimate=cost(24 * len(jobs) * width * width * 40, 2 * len(jobs) * width * width),
    )(coords, *after)


def redatum_kernel(reach, below, wave, above, taps, *refs):
    out, padded = refs[-2:]
    count, width = wave.shape
    edge = below.shape[1]
    blocks = width // LANES
    halves = range(count // LANES)

    def fill(lane, source, x, start):
        held = slice(lane * LANES, (lane + 1) * LANES)
        block = source[held, pl.ds(x, LANES)].astype(jnp.float32)
        padded[lane, pl.ds(start, LANES), :] = block.T

    for lane in halves:
        held = slice(lane * LANES, (lane + 1) * LANES)
        fill(lane, below, 0, 0)
        fill(lane, above, 0, edge + width)
        for k in range(min(2, blocks)):
            fill(lane, wave, k * LANES, edge + k * LANES)

        @pl.loop(0, blocks)
        def _(block):
            base = pl.multiple_of(block * LANES, LANES)
            total = None
            for j in range(taps.shape[0]):
                weight = jnp.broadcast_to(taps[j : j + 1, held], (LANES, LANES))
                term = weight * padded[lane, pl.ds(base + edge - reach + j, LANES), :]
                total = term if total is None else total + term
            out[held, pl.ds(base, LANES)] = total.T.astype(out.dtype)
            ahead = pl.multiple_of(jnp.minimum(block + 2, blocks - 1) * LANES, LANES)
            fill(lane, wave, ahead, edge + ahead)


def redatum(below, wave, above, taps, *after):
    count, width = wave.shape
    reach = (taps.shape[0] - 1) // 2
    long = width + 2 * below.shape[1]
    return pl.pallas_call(
        functools.partial(redatum_kernel, reach),
        out_shape=jax.ShapeDtypeStruct((count, width), jnp.bfloat16),
        in_specs=[VMEM] * 4 + [ANY] * len(after),
        out_specs=VMEM,
        scratch_shapes=[pltpu.VMEM((count // LANES, long, LANES), jnp.float32)],
        compiler_params=params(6),
        cost_estimate=cost(24 * 2 * width * width * 60, count * width * 4),
        name="redatum",
    )(below, wave, above, taps, *after)


def mix_kernel(held, mine, theirs, near, far, *refs):
    out = refs[-1]
    width = near.shape[1]
    scale = SCALE / math.sqrt(width)
    step = min(width, 256)
    for c in range(0, width, step):
        columns = slice(c, c + step)
        total = jnp.dot(mine[held, :], near[:, columns], preferred_element_type=jnp.float32)
        total += jnp.dot(theirs[held, :], far[:, columns], preferred_element_type=jnp.float32)
        out[:, columns] = (total * scale).astype(out.dtype)


def mix(part, mine, theirs, near, far, *after):
    count, width = mine.shape
    held = slice(part * LANES, (part + 1) * LANES) if count > LANES else slice(0, LANES)
    return pl.pallas_call(
        functools.partial(mix_kernel, held),
        out_shape=jax.ShapeDtypeStruct((LANES, width), jnp.bfloat16),
        in_specs=[VMEM] * 4 + [ANY] * len(after),
        out_specs=VMEM,
        compiler_params=params(7),
        cost_estimate=cost(24 * width * width * 15, 4 * width * width),
        name="mix",
    )(mine, theirs, near, far, *after)


def last_kernel(part, state, near, far, own_mask, far_mask, *refs):
    own, other = refs[-2:]
    width = near.shape[1]
    scale = SCALE / math.sqrt(width)
    step = min(width, 256)
    held = slice(part * LANES, (part + 1) * LANES)
    for k, (table, mask, out) in enumerate(((far, far_mask, other), (near, own_mask, own))):
        for c in range(0, width, step):
            columns = slice(c, c + step)
            mixed = jnp.dot(state[...], table[:, columns], preferred_element_type=jnp.float32)
            kept = jnp.where(mask[held, columns].astype(jnp.float32) > 0, mixed, 0.0)
            total = jnp.sum(kept, 0, keepdims=True) * scale
            if part > 0:
                total = total + refs[1 - k][:, columns]
            out[:, columns] = total


def last(part, state, near, far, own_mask, far_mask, sums, *after):
    count, width = state.shape
    shape = jax.ShapeDtypeStruct((1, width), jnp.float32)
    return pl.pallas_call(
        functools.partial(last_kernel, part),
        out_shape=(shape, shape),
        in_specs=[VMEM] * (5 + len(sums)) + [ANY] * len(after),
        out_specs=(VMEM, VMEM),
        compiler_params=params(8),
        cost_estimate=cost(4 * count * width * width, 4 * width * width),
    )(state, near, far, own_mask, far_mask, *sums, *after)


def on_device(wavefield, redatum_taps, cell_x, cell_depth, slowness, illumination, aperture):
    index = lax.axis_index("space")
    blocks = lax.axis_size("space") // BOXES
    block_bits = blocks.bit_length() - 1
    box = index // blocks
    block = index % blocks
    count, width = wavefield.shape
    depth = cell_depth.reshape(BOXES * width // LANES, LANES)
    head, tail, mask, coords = prepare(blocks, wavefield, aperture, cell_x, depth, slowness)
    below = passed_along(tail, "space", blocks)
    above = passed_along(head, "space", -blocks)
    taps = redatum_taps
    if blocks > 1:
        taps = lax.dynamic_slice_in_dim(redatum_taps, block * count, count, 0)
    taps = taps.T
    parts = range(count // LANES)

    (near,) = tables(0, (0,), coords)
    below, above, held_mask = lax.optimization_barrier((below, above, mask))
    masks = partner(held_mask, "space", LEVELS - 1 + block_bits)
    state = redatum(below, wavefield, above, taps, near)
    received = partner(state, "space", block_bits)
    (far,) = tables(0, (1,), coords, state)
    states = [state for _ in parts]
    theirs = [received for _ in parts]
    table, ahead = (near, far), far
    for level in range(LEVELS - 1):
        for part in parts:
            states[part] = mix(part, states[part], theirs[part], *table, ahead)
            ahead = states[part]
            if level + 2 < LEVELS:
                theirs[part] = partner(states[part], "space", level + 1 + block_bits)
            if part == (len(parts) - 1 if level == 0 else 0):
                following = tables(level + 1, (0, 1), coords, ahead)
                ahead = following[0]
        table = following
    sums = ()
    for part in parts:
        sums = last(part, states[part], *table, mask, masks, sums)
    own, other = sums
    summed = own + partner(other, "space", LEVELS - 1 + block_bits)
    weights = lax.dynamic_slice_in_dim(illumination, box * width, width)
    image = summed * weights[None] / jnp.sqrt(jnp.float32(count * blocks))
    for level in range(block_bits):
        image = image + partner(image, "space", level)
    share = width // blocks
    return lax.dynamic_slice_in_dim(image, block * share, share, 1)


def solution(mesh):
    placed = (
        P(("groups", "space"), None),
        P("groups", None),
        P(),
        P(),
        P(),
        P("groups"),
        P(("groups", "space"), None),
    )
    return jax.shard_map(
        on_device,
        mesh=mesh,
        in_specs=placed,
        out_specs=P(("groups", "space"), None),
        check_vma=False,
    )
```

```python
import functools
import math

import jax
import jax.numpy as jnp
from jax import lax
from jax.experimental import pallas as pl
from jax.experimental.pallas import tpu as pltpu
from jax.sharding import PartitionSpec as P


LEVELS = 4
BOXES = 16
LANES = 128

POLY_A = -0.55846636
POLY_B = 0.08535978
SCALE = -73.58594804
VMEM = pl.BlockSpec(memory_space=pltpu.VMEM)
GRANT = 56 << 20
ANY = pl.BlockSpec(memory_space=pl.ANY)
HBM = pl.BlockSpec(memory_space=pltpu.HBM)
SMEM = pl.BlockSpec(memory_space=pltpu.SMEM)


def params(mib):
    return pltpu.CompilerParams(vmem_limit_bytes=mib << 20)


def cost(flops, moved, transcendentals=0):
    return pl.CostEstimate(flops=flops, bytes_accessed=moved, transcendentals=transcendentals)


def across(shard, axis, blocks):
    devices = lax.axis_size(axis)
    shift = [blocks if i // blocks % 2 else -blocks for i in range(devices)]
    pairs = [(i, i + by) for i, by in enumerate(shift) if 0 <= i + by < devices]
    return lax.ppermute(shard, axis, pairs)


def partner(shard, axis, bit):
    return lax.ppermute(shard, axis, [(i, i ^ 1 << bit) for i in range(lax.axis_size(axis))])


def cosine(squared):
    u = squared * lax.rsqrt(squared)
    r = u - jnp.round(u)
    w = jnp.abs(r) - 0.25
    q = w * w
    return w * ((q + POLY_A) * q + POLY_B)


def boxes_of(level, blocks):
    box = lax.axis_index("space") // blocks
    bit = 1 << level
    upper = (box // bit) % 2
    return box, box + bit - 2 * bit * upper


ROW, OTHER_ROW, COLUMN, BELOW, OTHER_COLUMN, OTHER_BELOW = range(6)


def prepare_kernel(blocks, wave, aperture, cell_x, depth, slowness, *refs):
    near_edge, far_edge, mask, coords, cells, depths, slow, marks, sems = refs
    width = wave.shape[1]
    tall = width // LANES
    box = boxes_of(0, blocks)[0]
    others = [boxes_of(level, blocks)[1] for level in range(LEVELS)]
    copies = [pltpu.make_async_copy(slowness, slow, sems.at[0])]
    for k, which in enumerate([box] + others):
        at = pl.ds(pl.multiple_of(which * width, width), width)
        copies.append(pltpu.make_async_copy(cell_x.at[:, at], cells.at[k], sems.at[1 + k]))
    for k, which in enumerate((box, others[-1])):
        at = pl.ds(pl.multiple_of(which * tall, tall), tall)
        copies.append(pltpu.make_async_copy(depth.at[at, :], depths.at[k], sems.at[6 + k]))
    end = width - LANES
    even = 1 - box % 2
    first = pl.ds(pl.multiple_of(even * end, LANES), LANES)
    second = pl.ds(pl.multiple_of((1 - even) * end, LANES), LANES)
    late = [
        pltpu.make_async_copy(wave.at[:, first], near_edge, sems.at[8]),
        pltpu.make_async_copy(wave.at[:, second], far_edge, sems.at[9]),
        pltpu.make_async_copy(aperture, marks, sems.at[10]),
    ]
    for copy in copies + late:
        copy.start()
    for copy in copies:
        copy.wait()
    coords[...] = jnp.zeros_like(coords)
    for level in range(LEVELS):
        turns = slow[level] * (0.5 / math.pi)
        base = 8 * level

        def put(kind, source, row):
            coords[base + kind : base + kind + 1, :] = (
                cells[source, row : row + 1, :].astype(jnp.float32) * turns
            )

        def put_below(kind, source):
            for k in range(tall):
                part = depths[source, k : k + 1, :].astype(jnp.float32) * turns
                coords[base + kind : base + kind + 1, k * LANES : (k + 1) * LANES] = part * part

        put(ROW, 0, level)
        put(OTHER_ROW, 1 + level, level)
        put(COLUMN, 0, level + 1)
        put_below(BELOW, 0)
        if level + 1 == LEVELS:
            put(OTHER_COLUMN, LEVELS, level + 1)
            put_below(OTHER_BELOW, 1)
    for copy in late:
        copy.wait()
    mask[...] = (marks[...] > 0).astype(jnp.float32).astype(jnp.bfloat16)


def prepare(blocks, wave, aperture, cell_x, depth, slowness):
    count, width = wave.shape
    levels = cell_x.shape[0]
    edge = jax.ShapeDtypeStruct((count, LANES), wave.dtype)
    return pl.pallas_call(
        functools.partial(prepare_kernel, blocks),
        out_shape=(
            edge,
            edge,
            jax.ShapeDtypeStruct((count, width), jnp.bfloat16),
            jax.ShapeDtypeStruct((8 * LEVELS, width), jnp.float32),
        ),
        in_specs=[HBM] * 5,
        out_specs=(VMEM,) * 4,
        scratch_shapes=[
            pltpu.VMEM((1 + LEVELS, levels, width), jnp.int32),
            pltpu.VMEM((2, width // LANES, LANES), jnp.int32),
            pltpu.SMEM((LEVELS,), jnp.float32),
            pltpu.VMEM((count, width), jnp.int32),
            pltpu.SemaphoreType.DMA((11,)),
        ],
        compiler_params=pltpu.CompilerParams(vmem_limit_bytes=GRANT),
        cost_estimate=cost(24 * 2 * width * width * 15, count * width * 8),
        name="prepare",
    )(wave, aperture, cell_x, depth, slowness)


def tables_kernel(jobs, step, coords, *refs):
    outs, rows = refs[-1 - len(jobs) : -1], refs[-1]
    width = outs[0].shape[0]
    steps = width // step

    def fill(slot, row, i):
        at = pl.ds(pl.multiple_of(i * step, step), step)
        rows[slot] = jnp.broadcast_to(coords[row : row + 1, at], (LANES, step)).T

    for (row, column, below), out in zip(jobs, outs):
        fill(0, row, 0)

        @pl.loop(0, steps)
        def _(i):
            at = pl.ds(pl.multiple_of(i * step, step), step)
            part = rows[i % 2]
            part = jnp.concatenate([part, part], 1)
            for c in range(0, width, 2 * LANES):
                columns = slice(c, c + 2 * LANES)
                across = part - coords[column : column + 1, columns]
                squared = across * across + coords[below : below + 1, columns]
                out[at, columns] = cosine(squared).astype(jnp.bfloat16)
            fill((i + 1) % 2, row, jnp.minimum(i + 1, steps - 1))


def tables(level, which, coords, *after):
    width = coords.shape[1]
    base = 8 * level
    near = (base + ROW, base + COLUMN, base + BELOW)
    far = (base + OTHER_ROW, base + COLUMN, base + BELOW)
    if level + 1 == LEVELS:
        far = (base + ROW, base + OTHER_COLUMN, base + OTHER_BELOW)
    jobs = [(near, far)[k] for k in which]
    shape = jax.ShapeDtypeStruct((width, width), jnp.bfloat16)
    step = LANES
    return pl.pallas_call(
        functools.partial(tables_kernel, jobs, step),
        out_shape=(shape,) * len(jobs),
        in_specs=[VMEM] + [ANY] * len(after),
        out_specs=(VMEM,) * len(jobs),
        scratch_shapes=[pltpu.VMEM((2, step, LANES), jnp.float32)],
        compiler_params=params(6),
        cost_estimate=cost(24 * len(jobs) * width * width * 40, 2 * len(jobs) * width * width),
    )(coords, *after)


def redatum_kernel(reach, blocks, near_edge, wave, far_edge, taps, *refs):
    out, padded = refs[-2:]
    count, width = wave.shape
    edge = near_edge.shape[1]
    even = 1 - boxes_of(0, blocks)[0] % 2
    after = edge + width
    starts = (pl.multiple_of(even * after, LANES), pl.multiple_of((1 - even) * after, LANES))
    for lane in range(count // LANES):
        held = slice(lane * LANES, (lane + 1) * LANES)
        for source, start in ((near_edge, starts[0]), (far_edge, starts[1]), (wave, edge)):
            for x in range(0, source.shape[1], LANES):
                block = source[held, x : x + LANES].astype(jnp.float32)
                padded[lane, pl.ds(start + x, LANES), :] = block.T

        @pl.loop(0, width // LANES)
        def _(block):
            base = pl.multiple_of(block * LANES, LANES)
            total = None
            for j in range(taps.shape[0]):
                weight = jnp.broadcast_to(taps[j : j + 1, held], (LANES, LANES))
                term = weight * padded[lane, pl.ds(base + edge - reach + j, LANES), :]
                total = term if total is None else total + term
            out[held, pl.ds(base, LANES)] = total.T.astype(out.dtype)


def redatum(blocks, near_edge, wave, far_edge, taps, *after):
    count, width = wave.shape
    reach = (taps.shape[0] - 1) // 2
    long = width + 2 * near_edge.shape[1]
    return pl.pallas_call(
        functools.partial(redatum_kernel, reach, blocks),
        out_shape=jax.ShapeDtypeStruct((count, width), jnp.bfloat16),
        in_specs=[VMEM] * 4 + [ANY] * len(after),
        out_specs=VMEM,
        scratch_shapes=[pltpu.VMEM((count // LANES, long, LANES), jnp.float32)],
        compiler_params=params(6),
        cost_estimate=cost(24 * 2 * width * width * 60, count * width * 4),
        name="redatum",
    )(near_edge, wave, far_edge, taps, *after)


def mix_kernel(held, mine, theirs, near, far, *refs):
    out = refs[-1]
    width = near.shape[1]
    scale = SCALE / math.sqrt(width)
    step = min(width, 256)
    for c in range(0, width, step):
        columns = slice(c, c + step)
        total = jnp.dot(mine[held, :], near[:, columns], preferred_element_type=jnp.float32)
        total += jnp.dot(theirs[held, :], far[:, columns], preferred_element_type=jnp.float32)
        out[:, columns] = (total * scale).astype(out.dtype)


def mix(part, mine, theirs, near, far, *after):
    count, width = mine.shape
    held = slice(part * LANES, (part + 1) * LANES) if count > LANES else slice(0, LANES)
    return pl.pallas_call(
        functools.partial(mix_kernel, held),
        out_shape=jax.ShapeDtypeStruct((LANES, width), jnp.bfloat16),
        in_specs=[VMEM] * 4 + [ANY] * len(after),
        out_specs=VMEM,
        compiler_params=params(7),
        cost_estimate=cost(24 * width * width * 15, 4 * width * width),
        name="mix",
    )(mine, theirs, near, far, *after)


def last_kernel(part, count, added, state, *refs):
    tables, masks, sums = refs[:count], refs[count : 2 * count], refs[2 * count : 2 * count + added]
    width = tables[0].shape[1]
    scale = SCALE / math.sqrt(width)
    step = min(width, 256)
    held = slice(part * LANES, (part + 1) * LANES)
    for k, out in enumerate(refs[-count:]):
        for c in range(0, width, step):
            columns = slice(c, c + step)
            mixed = jnp.dot(state[...], tables[k][:, columns], preferred_element_type=jnp.float32)
            kept = jnp.where(masks[k][held, columns].astype(jnp.float32) > 0, mixed, 0.0)
            total = jnp.sum(kept, 0, keepdims=True) * scale
            if added:
                total = total + sums[k][:, columns]
            out[:, columns] = total


def last(part, state, tables, masks, sums, *after):
    width = state.shape[1]
    count = len(tables)
    shape = jax.ShapeDtypeStruct((1, width), jnp.float32)
    return pl.pallas_call(
        functools.partial(last_kernel, part, count, len(sums)),
        out_shape=(shape,) * count,
        in_specs=[VMEM] * (1 + 2 * count + len(sums)) + [ANY] * len(after),
        out_specs=(VMEM,) * count,
        compiler_params=params(7),
        cost_estimate=cost(24 * count * width * width * 8, 2 * count * width * width),
    )(state, *tables, *masks, *sums, *after)


def on_device(wavefield, redatum_taps, cell_x, cell_depth, slowness, illumination, aperture):
    index = lax.axis_index("space")
    blocks = lax.axis_size("space") // BOXES
    block_bits = blocks.bit_length() - 1
    box = index // blocks
    block = index % blocks
    count, width = wavefield.shape
    depth = cell_depth.reshape(BOXES * width // LANES, LANES)
    near_edge, far_edge, mask, coords = prepare(
        blocks, wavefield, aperture, cell_x, depth, slowness
    )
    near_edge = partner(near_edge, "space", block_bits)
    far_edge = across(far_edge, "space", blocks)
    taps = redatum_taps
    if blocks > 1:
        taps = lax.dynamic_slice_in_dim(redatum_taps, block * count, count, 0)
    taps = taps.T
    parts = range(count // LANES)

    (near,) = tables(0, (0,), coords)
    near_edge, far_edge, held_mask = lax.optimization_barrier((near_edge, far_edge, mask))
    masks = partner(held_mask, "space", LEVELS - 1 + block_bits)
    state = redatum(blocks, near_edge, wavefield, far_edge, taps, near)
    received = partner(state, "space", block_bits)
    (far,) = tables(0, (1,), coords, state)
    states = [state for _ in parts]
    theirs = [received for _ in parts]
    table, ahead = (near, far), far
    both, sums = (mask, masks), ()
    for level in range(LEVELS - 1):
        for part in parts:
            states[part] = mix(part, states[part], theirs[part], *table, ahead)
            ahead = states[part]
            if level + 2 == LEVELS and part + 1 < len(parts):
                sums = last(part, states[part], later, both, sums)
                ahead = sums[0]
            if level + 2 == LEVELS and part + 1 == len(parts):
                (other,) = last(part, states[part], later[1:], both[1:], sums[1:])
                (own,) = last(part, states[part], later[:1], both[:1], sums[:1], other)
            if level + 2 < LEVELS:
                theirs[part] = partner(states[part], "space", level + 1 + block_bits)
            if part == (0 if level == 1 else len(parts) - 1) and level < 2:
                following = tables(level + 1, (0, 1), coords, ahead)
                ahead = following[0]
            if part == len(parts) - 1 and level == 1:
                later = tables(level + 2, (0, 1), coords, ahead)
                ahead = later[0]
        table = following
    summed = own + partner(other, "space", LEVELS - 1 + block_bits)
    weights = lax.dynamic_slice_in_dim(illumination, box * width, width)
    image = summed * weights[None] / jnp.sqrt(jnp.float32(count * blocks))
    for level in range(block_bits):
        image = image + partner(image, "space", level)
    share = width // blocks
    return lax.dynamic_slice_in_dim(image, block * share, share, 1)


def solution(mesh):
    placed = (
        P(("groups", "space"), None),
        P("groups", None),
        P(),
        P(),
        P(),
        P("groups"),
        P(("groups", "space"), None),
    )
    return jax.shard_map(
        on_device,
        mesh=mesh,
        in_specs=placed,
        out_specs=P(("groups", "space"), None),
        check_vma=False,
    )
```

```python
import functools
import math

import jax
import jax.numpy as jnp
from jax import lax
from jax.experimental import pallas as pl
from jax.experimental.pallas import tpu as pltpu
from jax.sharding import PartitionSpec as P


LEVELS = 4
BOXES = 16
LANES = 128

POLY_A = -0.55846636
POLY_B = 0.08535978
SCALE = -73.58594804
VMEM = pl.BlockSpec(memory_space=pltpu.VMEM)
GRANT = 56 << 20
ANY = pl.BlockSpec(memory_space=pl.ANY)
HBM = pl.BlockSpec(memory_space=pltpu.HBM)
SMEM = pl.BlockSpec(memory_space=pltpu.SMEM)


def params(mib):
    return pltpu.CompilerParams(vmem_limit_bytes=mib << 20)


def cost(flops, moved, transcendentals=0):
    return pl.CostEstimate(flops=flops, bytes_accessed=moved, transcendentals=transcendentals)


def across(shard, axis, blocks):
    devices = lax.axis_size(axis)
    shift = [blocks if i // blocks % 2 else -blocks for i in range(devices)]
    pairs = [(i, i + by) for i, by in enumerate(shift) if 0 <= i + by < devices]
    return lax.ppermute(shard, axis, pairs)


def partner(shard, axis, bit):
    return lax.ppermute(shard, axis, [(i, i ^ 1 << bit) for i in range(lax.axis_size(axis))])


def cosine(squared):
    u = squared * lax.rsqrt(squared)
    r = u - jnp.round(u)
    w = jnp.abs(r) - 0.25
    q = w * w
    return w * ((q + POLY_A) * q + POLY_B)


def boxes_of(level, blocks):
    box = lax.axis_index("space") // blocks
    bit = 1 << level
    upper = (box // bit) % 2
    return box, box + bit - 2 * bit * upper


ROW, OTHER_ROW, COLUMN, BELOW, OTHER_COLUMN, OTHER_BELOW, WEIGHT, OTHER_WEIGHT = range(8)


def prepare_kernel(blocks, wave, aperture, cell_x, depth, illumination, slowness, *refs):
    near_edge, far_edge, mask, coords, cells, depths, lights, slow, marks, sems = refs
    width = wave.shape[1]
    tall = width // LANES
    box = boxes_of(0, blocks)[0]
    others = [boxes_of(level, blocks)[1] for level in range(LEVELS)]
    copies = [pltpu.make_async_copy(slowness, slow, sems.at[0])]
    for k, which in enumerate([box] + others):
        at = pl.ds(pl.multiple_of(which * width, width), width)
        copies.append(pltpu.make_async_copy(cell_x.at[:, at], cells.at[k], sems.at[1 + k]))
    for k, which in enumerate((box, others[-1])):
        at = pl.ds(pl.multiple_of(which * tall, tall), tall)
        copies.append(pltpu.make_async_copy(depth.at[at, :], depths.at[k], sems.at[6 + k]))
        light = illumination.at[at, :]
        copies.append(pltpu.make_async_copy(light, lights.at[k], sems.at[11 + k]))
    end = width - LANES
    even = 1 - box % 2
    first = pl.ds(pl.multiple_of(even * end, LANES), LANES)
    second = pl.ds(pl.multiple_of((1 - even) * end, LANES), LANES)
    late = [
        pltpu.make_async_copy(wave.at[:, first], near_edge, sems.at[8]),
        pltpu.make_async_copy(wave.at[:, second], far_edge, sems.at[9]),
        pltpu.make_async_copy(aperture, marks, sems.at[10]),
    ]
    for copy in copies + late:
        copy.start()
    for copy in copies:
        copy.wait()
    coords[...] = jnp.zeros_like(coords)
    for level in range(LEVELS):
        turns = slow[level] * (0.5 / math.pi)
        base = 8 * level

        def put(kind, source, row):
            coords[base + kind : base + kind + 1, :] = (
                cells[source, row : row + 1, :].astype(jnp.float32) * turns
            )

        def put_below(kind, source):
            for k in range(tall):
                part = depths[source, k : k + 1, :].astype(jnp.float32) * turns
                coords[base + kind : base + kind + 1, k * LANES : (k + 1) * LANES] = part * part

        put(ROW, 0, level)
        put(OTHER_ROW, 1 + level, level)
        put(COLUMN, 0, level + 1)
        put_below(BELOW, 0)
        if level + 1 == LEVELS:
            put(OTHER_COLUMN, LEVELS, level + 1)
            put_below(OTHER_BELOW, 1)
    share = 1.0 / math.sqrt(wave.shape[0] * blocks)
    base = 8 * (LEVELS - 1)
    for source, kind in enumerate((WEIGHT, OTHER_WEIGHT)):
        for k in range(tall):
            coords[base + kind : base + kind + 1, k * LANES : (k + 1) * LANES] = (
                lights[source, k : k + 1, :] * share
            )
    for copy in late:
        copy.wait()
    mask[...] = (marks[...] > 0).astype(jnp.float32).astype(jnp.bfloat16)


def prepare(blocks, wave, aperture, cell_x, depth, illumination, slowness):
    count, width = wave.shape
    levels = cell_x.shape[0]
    edge = jax.ShapeDtypeStruct((count, LANES), wave.dtype)
    return pl.pallas_call(
        functools.partial(prepare_kernel, blocks),
        out_shape=(
            edge,
            edge,
            jax.ShapeDtypeStruct((count, width), jnp.bfloat16),
            jax.ShapeDtypeStruct((8 * LEVELS, width), jnp.float32),
        ),
        in_specs=[HBM] * 6,
        out_specs=(VMEM,) * 4,
        scratch_shapes=[
            pltpu.VMEM((1 + LEVELS, levels, width), jnp.int32),
            pltpu.VMEM((2, width // LANES, LANES), jnp.int32),
            pltpu.VMEM((2, width // LANES, LANES), jnp.float32),
            pltpu.SMEM((LEVELS,), jnp.float32),
            pltpu.VMEM((count, width), jnp.int32),
            pltpu.SemaphoreType.DMA((13,)),
        ],
        compiler_params=pltpu.CompilerParams(vmem_limit_bytes=GRANT),
        cost_estimate=cost(24 * 2 * width * width * 15, count * width * 8),
        name="prepare",
    )(wave, aperture, cell_x, depth, illumination, slowness)


def tables_kernel(jobs, step, coords, *refs):
    outs, rows = refs[-1 - len(jobs) : -1], refs[-1]
    width = outs[0].shape[0]
    steps = width // step

    def fill(slot, row, i):
        at = pl.ds(pl.multiple_of(i * step, step), step)
        rows[slot] = jnp.broadcast_to(coords[row : row + 1, at], (LANES, step)).T

    for (row, column, below), out in zip(jobs, outs):
        fill(0, row, 0)

        @pl.loop(0, steps)
        def _(i):
            at = pl.ds(pl.multiple_of(i * step, step), step)
            part = rows[i % 2]
            part = jnp.concatenate([part, part], 1)
            for c in range(0, width, 2 * LANES):
                columns = slice(c, c + 2 * LANES)
                across = part - coords[column : column + 1, columns]
                squared = across * across + coords[below : below + 1, columns]
                out[at, columns] = cosine(squared).astype(jnp.bfloat16)
            fill((i + 1) % 2, row, jnp.minimum(i + 1, steps - 1))


def tables(level, which, coords, *after):
    width = coords.shape[1]
    base = 8 * level
    near = (base + ROW, base + COLUMN, base + BELOW)
    far = (base + OTHER_ROW, base + COLUMN, base + BELOW)
    if level + 1 == LEVELS:
        far = (base + ROW, base + OTHER_COLUMN, base + OTHER_BELOW)
    jobs = [(near, far)[k] for k in which]
    shape = jax.ShapeDtypeStruct((width, width), jnp.bfloat16)
    step = LANES
    return pl.pallas_call(
        functools.partial(tables_kernel, jobs, step),
        out_shape=(shape,) * len(jobs),
        in_specs=[VMEM] + [ANY] * len(after),
        out_specs=(VMEM,) * len(jobs),
        scratch_shapes=[pltpu.VMEM((2, step, LANES), jnp.float32)],
        compiler_params=params(6),
        cost_estimate=cost(24 * len(jobs) * width * width * 40, 2 * len(jobs) * width * width),
    )(coords, *after)


def redatum_kernel(reach, blocks, near_edge, wave, far_edge, taps, *refs):
    out, padded = refs[-2:]
    count, width = wave.shape
    edge = near_edge.shape[1]
    even = 1 - boxes_of(0, blocks)[0] % 2
    after = edge + width
    starts = (pl.multiple_of(even * after, LANES), pl.multiple_of((1 - even) * after, LANES))
    for lane in range(count // LANES):
        held = slice(lane * LANES, (lane + 1) * LANES)
        for source, start in ((near_edge, starts[0]), (far_edge, starts[1]), (wave, edge)):
            for x in range(0, source.shape[1], LANES):
                block = source[held, x : x + LANES].astype(jnp.float32)
                padded[lane, pl.ds(start + x, LANES), :] = block.T

        @pl.loop(0, width // LANES)
        def _(block):
            base = pl.multiple_of(block * LANES, LANES)
            total = None
            for j in range(taps.shape[0]):
                weight = jnp.broadcast_to(taps[j : j + 1, held], (LANES, LANES))
                term = weight * padded[lane, pl.ds(base + edge - reach + j, LANES), :]
                total = term if total is None else total + term
            out[held, pl.ds(base, LANES)] = total.T.astype(out.dtype)


def redatum(blocks, near_edge, wave, far_edge, taps, *after):
    count, width = wave.shape
    reach = (taps.shape[0] - 1) // 2
    long = width + 2 * near_edge.shape[1]
    return pl.pallas_call(
        functools.partial(redatum_kernel, reach, blocks),
        out_shape=jax.ShapeDtypeStruct((count, width), jnp.bfloat16),
        in_specs=[VMEM] * 4 + [ANY] * len(after),
        out_specs=VMEM,
        scratch_shapes=[pltpu.VMEM((count // LANES, long, LANES), jnp.float32)],
        compiler_params=params(6),
        cost_estimate=cost(24 * 2 * width * width * 60, count * width * 4),
        name="redatum",
    )(near_edge, wave, far_edge, taps, *after)


def mix_kernel(held, mine, theirs, near, far, *refs):
    out = refs[-1]
    width = near.shape[1]
    scale = SCALE / math.sqrt(width)
    step = min(width, 256)
    for c in range(0, width, step):
        columns = slice(c, c + step)
        total = jnp.dot(mine[held, :], near[:, columns], preferred_element_type=jnp.float32)
        total += jnp.dot(theirs[held, :], far[:, columns], preferred_element_type=jnp.float32)
        out[:, columns] = (total * scale).astype(out.dtype)


def mix(part, mine, theirs, near, far, *after):
    count, width = mine.shape
    held = slice(part * LANES, (part + 1) * LANES) if count > LANES else slice(0, LANES)
    return pl.pallas_call(
        functools.partial(mix_kernel, held),
        out_shape=jax.ShapeDtypeStruct((LANES, width), jnp.bfloat16),
        in_specs=[VMEM] * 4 + [ANY] * len(after),
        out_specs=VMEM,
        compiler_params=params(7),
        cost_estimate=cost(24 * width * width * 15, 4 * width * width),
        name="mix",
    )(mine, theirs, near, far, *after)


def last_kernel(part, weights, added, state, coords, *refs):
    count = len(weights)
    tables, masks, sums = refs[:count], refs[count : 2 * count], refs[2 * count : 2 * count + added]
    width = tables[0].shape[1]
    scale = SCALE / math.sqrt(width)
    step = min(width, 256)
    held = slice(part * LANES, (part + 1) * LANES)
    for k, out in enumerate(refs[-count:]):
        for c in range(0, width, step):
            columns = slice(c, c + step)
            mixed = jnp.dot(state[...], tables[k][:, columns], preferred_element_type=jnp.float32)
            kept = jnp.where(masks[k][held, columns].astype(jnp.float32) > 0, mixed, 0.0)
            total = jnp.sum(kept, 0, keepdims=True) * scale
            total = total * coords[weights[k] : weights[k] + 1, columns]
            if added:
                total = total + sums[k][:, columns]
            out[:, columns] = total


def last(part, which, state, coords, tables, masks, sums, *after):
    width = state.shape[1]
    count = len(which)
    base = 8 * (LEVELS - 1)
    weights = [base + (WEIGHT, OTHER_WEIGHT)[k] for k in which]
    tables, masks = [tables[k] for k in which], [masks[k] for k in which]
    shape = jax.ShapeDtypeStruct((1, width), jnp.float32)
    return pl.pallas_call(
        functools.partial(last_kernel, part, weights, len(sums)),
        out_shape=(shape,) * count,
        in_specs=[VMEM] * (2 + 2 * count + len(sums)) + [ANY] * len(after),
        out_specs=(VMEM,) * count,
        compiler_params=params(7),
        cost_estimate=cost(24 * count * width * width * 8, 2 * count * width * width),
    )(state, coords, *tables, *masks, *sums, *after)


def on_device(wavefield, redatum_taps, cell_x, cell_depth, slowness, illumination, aperture):
    index = lax.axis_index("space")
    blocks = lax.axis_size("space") // BOXES
    block_bits = blocks.bit_length() - 1
    block = index % blocks
    count, width = wavefield.shape
    depth = cell_depth.reshape(BOXES * width // LANES, LANES)
    light = illumination.reshape(BOXES * width // LANES, LANES)
    near_edge, far_edge, mask, coords = prepare(
        blocks, wavefield, aperture, cell_x, depth, light, slowness
    )
    near_edge = partner(near_edge, "space", block_bits)
    far_edge = across(far_edge, "space", blocks)
    taps = redatum_taps
    if blocks > 1:
        taps = lax.dynamic_slice_in_dim(redatum_taps, block * count, count, 0)
    taps = taps.T
    parts = range(count // LANES)

    (near,) = tables(0, (0,), coords)
    near_edge, far_edge, held_mask = lax.optimization_barrier((near_edge, far_edge, mask))
    masks = partner(held_mask, "space", LEVELS - 1 + block_bits)
    state = redatum(blocks, near_edge, wavefield, far_edge, taps, near)
    received = partner(state, "space", block_bits)
    (far,) = tables(0, (1,), coords, state)
    states = [state for _ in parts]
    theirs = [received for _ in parts]
    table, ahead = (near, far), far
    both, sums = (mask, masks), ()
    for level in range(LEVELS - 1):
        for part in parts:
            states[part] = mix(part, states[part], theirs[part], *table, ahead)
            ahead = states[part]
            if level + 2 == LEVELS and part + 1 < len(parts):
                sums = last(part, (0, 1), states[part], coords, later, both, sums)
                ahead = sums[0]
            if level + 2 == LEVELS and part + 1 == len(parts):
                final = (states[part], coords, later, both)
                (other,) = last(part, (1,), *final, sums[1:])
                (own,) = last(part, (0,), *final, sums[:1], other)
            if level + 2 < LEVELS:
                theirs[part] = partner(states[part], "space", level + 1 + block_bits)
            if part == (0 if level == 1 else len(parts) - 1) and level < 2:
                following = tables(level + 1, (0, 1), coords, ahead)
                ahead = following[0]
            if part == len(parts) - 1 and level == 1:
                later = tables(level + 2, (0, 1), coords, ahead)
                ahead = later[0]
        table = following
    image = own + partner(other, "space", LEVELS - 1 + block_bits)
    for level in range(block_bits):
        image = image + partner(image, "space", level)
    share = width // blocks
    return lax.dynamic_slice_in_dim(image, block * share, share, 1)


def solution(mesh):
    placed = (
        P(("groups", "space"), None),
        P("groups", None),
        P(),
        P(),
        P(),
        P("groups"),
        P(("groups", "space"), None),
    )
    return jax.shard_map(
        on_device,
        mesh=mesh,
        in_specs=placed,
        out_specs=P(("groups", "space"), None),
        check_vma=False,
    )
```

```python
import functools
import math

import jax
import jax.numpy as jnp
from jax import lax
from jax.experimental import pallas as pl
from jax.experimental.pallas import tpu as pltpu
from jax.sharding import PartitionSpec as P


LEVELS = 4
BOXES = 16
LANES = 128

POLY_A = -0.55846636
POLY_B = 0.08535978
SCALE = -73.58594804
VMEM = pl.BlockSpec(memory_space=pltpu.VMEM)
GRANT = 56 << 20
ANY = pl.BlockSpec(memory_space=pl.ANY)
HBM = pl.BlockSpec(memory_space=pltpu.HBM)
SMEM = pl.BlockSpec(memory_space=pltpu.SMEM)


def params(mib):
    return pltpu.CompilerParams(vmem_limit_bytes=mib << 20)


def cost(flops, moved, transcendentals=0):
    return pl.CostEstimate(flops=flops, bytes_accessed=moved, transcendentals=transcendentals)


def across(shard, axis, blocks):
    devices = lax.axis_size(axis)
    shift = [blocks if i // blocks % 2 else -blocks for i in range(devices)]
    pairs = [(i, i + by) for i, by in enumerate(shift) if 0 <= i + by < devices]
    return lax.ppermute(shard, axis, pairs)


def partner(shard, axis, bit):
    return lax.ppermute(shard, axis, [(i, i ^ 1 << bit) for i in range(lax.axis_size(axis))])


def cosine(squared):
    u = squared * lax.rsqrt(squared)
    r = u - jnp.round(u)
    w = jnp.abs(r) - 0.25
    q = w * w
    return w * ((q + POLY_A) * q + POLY_B)


def boxes_of(level, blocks):
    box = lax.axis_index("space") // blocks
    bit = 1 << level
    upper = (box // bit) % 2
    return box, box + bit - 2 * bit * upper


ROW, OTHER_ROW, COLUMN, BELOW, OTHER_COLUMN, OTHER_BELOW, WEIGHT, OTHER_WEIGHT = range(8)


def prepare_kernel(blocks, wave, cell_x, depth, illumination, slowness, *refs):
    near_edge, far_edge, coords, cells, depths, lights, slow, sems = refs
    width = wave.shape[1]
    tall = width // LANES
    box = boxes_of(0, blocks)[0]
    others = [boxes_of(level, blocks)[1] for level in range(LEVELS)]
    copies = [pltpu.make_async_copy(slowness, slow, sems.at[0])]
    for k, which in enumerate([box] + others):
        at = pl.ds(pl.multiple_of(which * width, width), width)
        copies.append(pltpu.make_async_copy(cell_x.at[:, at], cells.at[k], sems.at[1 + k]))
    for k, which in enumerate((box, others[-1])):
        at = pl.ds(pl.multiple_of(which * tall, tall), tall)
        copies.append(pltpu.make_async_copy(depth.at[at, :], depths.at[k], sems.at[6 + k]))
        light = illumination.at[at, :]
        copies.append(pltpu.make_async_copy(light, lights.at[k], sems.at[10 + k]))
    end = width - LANES
    even = 1 - box % 2
    first = pl.ds(pl.multiple_of(even * end, LANES), LANES)
    second = pl.ds(pl.multiple_of((1 - even) * end, LANES), LANES)
    late = [
        pltpu.make_async_copy(wave.at[:, first], near_edge, sems.at[8]),
        pltpu.make_async_copy(wave.at[:, second], far_edge, sems.at[9]),
    ]
    for copy in copies + late:
        copy.start()
    for copy in copies:
        copy.wait()
    coords[...] = jnp.zeros_like(coords)
    for level in range(LEVELS):
        turns = slow[level] * (0.5 / math.pi)
        base = 8 * level

        def put(kind, source, row):
            coords[base + kind : base + kind + 1, :] = (
                cells[source, row : row + 1, :].astype(jnp.float32) * turns
            )

        def put_below(kind, source):
            for k in range(tall):
                part = depths[source, k : k + 1, :].astype(jnp.float32) * turns
                coords[base + kind : base + kind + 1, k * LANES : (k + 1) * LANES] = part * part

        put(ROW, 0, level)
        put(OTHER_ROW, 1 + level, level)
        put(COLUMN, 0, level + 1)
        put_below(BELOW, 0)
        if level + 1 == LEVELS:
            put(OTHER_COLUMN, LEVELS, level + 1)
            put_below(OTHER_BELOW, 1)
    share = 1.0 / math.sqrt(wave.shape[0] * blocks)
    base = 8 * (LEVELS - 1)
    for source, kind in enumerate((WEIGHT, OTHER_WEIGHT)):
        for k in range(tall):
            coords[base + kind : base + kind + 1, k * LANES : (k + 1) * LANES] = (
                lights[source, k : k + 1, :] * share
            )
    for copy in late:
        copy.wait()


def mark_kernel(aperture, mask):
    mask[...] = (aperture[...] > 0).astype(jnp.float32).astype(jnp.bfloat16)


def mark(aperture):
    return pl.pallas_call(
        mark_kernel,
        out_shape=jax.ShapeDtypeStruct(aperture.shape, jnp.bfloat16),
        in_specs=[VMEM],
        out_specs=VMEM,
        compiler_params=params(4),
        cost_estimate=cost(aperture.size * 200, aperture.size * 6),
        name="mark",
    )(aperture)


def prepare(blocks, wave, cell_x, depth, illumination, slowness):
    count, width = wave.shape
    levels = cell_x.shape[0]
    edge = jax.ShapeDtypeStruct((count, LANES), wave.dtype)
    return pl.pallas_call(
        functools.partial(prepare_kernel, blocks),
        out_shape=(
            edge,
            edge,
            jax.ShapeDtypeStruct((8 * LEVELS, width), jnp.float32),
        ),
        in_specs=[HBM] * 5,
        out_specs=(VMEM,) * 3,
        scratch_shapes=[
            pltpu.VMEM((1 + LEVELS, levels, width), jnp.int32),
            pltpu.VMEM((2, width // LANES, LANES), jnp.int32),
            pltpu.VMEM((2, width // LANES, LANES), jnp.float32),
            pltpu.SMEM((LEVELS,), jnp.float32),
            pltpu.SemaphoreType.DMA((12,)),
        ],
        compiler_params=pltpu.CompilerParams(vmem_limit_bytes=GRANT),
        cost_estimate=cost(24 * 2 * width * width * 15, count * width * 8),
        name="prepare",
    )(wave, cell_x, depth, illumination, slowness)


def tables_kernel(jobs, step, coords, *refs):
    outs, rows = refs[-1 - len(jobs) : -1], refs[-1]
    width = outs[0].shape[0]
    steps = width // step

    def fill(slot, row, i):
        at = pl.ds(pl.multiple_of(i * step, step), step)
        rows[slot] = jnp.broadcast_to(coords[row : row + 1, at], (LANES, step)).T

    for (row, column, below), out in zip(jobs, outs):
        fill(0, row, 0)

        @pl.loop(0, steps)
        def _(i):
            at = pl.ds(pl.multiple_of(i * step, step), step)
            part = rows[i % 2]
            part = jnp.concatenate([part, part], 1)
            for c in range(0, width, 2 * LANES):
                columns = slice(c, c + 2 * LANES)
                across = part - coords[column : column + 1, columns]
                squared = across * across + coords[below : below + 1, columns]
                out[at, columns] = cosine(squared).astype(jnp.bfloat16)
            fill((i + 1) % 2, row, jnp.minimum(i + 1, steps - 1))


def tables(level, which, coords, *after):
    width = coords.shape[1]
    base = 8 * level
    near = (base + ROW, base + COLUMN, base + BELOW)
    far = (base + OTHER_ROW, base + COLUMN, base + BELOW)
    if level + 1 == LEVELS:
        far = (base + ROW, base + OTHER_COLUMN, base + OTHER_BELOW)
    jobs = [(near, far)[k] for k in which]
    shape = jax.ShapeDtypeStruct((width, width), jnp.bfloat16)
    step = LANES
    return pl.pallas_call(
        functools.partial(tables_kernel, jobs, step),
        out_shape=(shape,) * len(jobs),
        in_specs=[VMEM] + [ANY] * len(after),
        out_specs=(VMEM,) * len(jobs),
        scratch_shapes=[pltpu.VMEM((2, step, LANES), jnp.float32)],
        compiler_params=params(6),
        cost_estimate=cost(24 * len(jobs) * width * width * 40, 2 * len(jobs) * width * width),
    )(coords, *after)


def redatum_kernel(reach, blocks, near_edge, wave, far_edge, taps, *refs):
    out, padded = refs[-2:]
    count, width = wave.shape
    edge = near_edge.shape[1]
    even = 1 - boxes_of(0, blocks)[0] % 2
    after = edge + width
    starts = (pl.multiple_of(even * after, LANES), pl.multiple_of((1 - even) * after, LANES))
    for lane in range(count // LANES):
        held = slice(lane * LANES, (lane + 1) * LANES)
        for source, start in ((near_edge, starts[0]), (far_edge, starts[1]), (wave, edge)):
            for x in range(0, source.shape[1], LANES):
                block = source[held, x : x + LANES].astype(jnp.float32)
                padded[lane, pl.ds(start + x, LANES), :] = block.T

        @pl.loop(0, width // LANES)
        def _(block):
            base = pl.multiple_of(block * LANES, LANES)
            total = None
            for j in range(taps.shape[0]):
                weight = jnp.broadcast_to(taps[j : j + 1, held], (LANES, LANES))
                term = weight * padded[lane, pl.ds(base + edge - reach + j, LANES), :]
                total = term if total is None else total + term
            out[held, pl.ds(base, LANES)] = total.T.astype(out.dtype)


def redatum(blocks, near_edge, wave, far_edge, taps, *after):
    count, width = wave.shape
    reach = (taps.shape[0] - 1) // 2
    long = width + 2 * near_edge.shape[1]
    return pl.pallas_call(
        functools.partial(redatum_kernel, reach, blocks),
        out_shape=jax.ShapeDtypeStruct((count, width), jnp.bfloat16),
        in_specs=[VMEM] * 4 + [ANY] * len(after),
        out_specs=VMEM,
        scratch_shapes=[pltpu.VMEM((count // LANES, long, LANES), jnp.float32)],
        compiler_params=params(6),
        cost_estimate=cost(24 * 2 * width * width * 60, count * width * 4),
        name="redatum",
    )(near_edge, wave, far_edge, taps, *after)


def mix_kernel(held, mine, theirs, near, far, *refs):
    out = refs[-1]
    width = near.shape[1]
    scale = SCALE / math.sqrt(width)
    step = min(width, 256)
    for c in range(0, width, step):
        columns = slice(c, c + step)
        total = jnp.dot(mine[held, :], near[:, columns], preferred_element_type=jnp.float32)
        total += jnp.dot(theirs[held, :], far[:, columns], preferred_element_type=jnp.float32)
        out[:, columns] = (total * scale).astype(out.dtype)


def mix(part, mine, theirs, near, far, *after):
    count, width = mine.shape
    held = slice(part * LANES, (part + 1) * LANES) if count > LANES else slice(0, LANES)
    return pl.pallas_call(
        functools.partial(mix_kernel, held),
        out_shape=jax.ShapeDtypeStruct((LANES, width), jnp.bfloat16),
        in_specs=[VMEM] * 4 + [ANY] * len(after),
        out_specs=VMEM,
        compiler_params=params(7),
        cost_estimate=cost(24 * width * width * 15, 4 * width * width),
        name="mix",
    )(mine, theirs, near, far, *after)


def last_kernel(part, weights, added, state, coords, *refs):
    count = len(weights)
    tables, masks, sums = refs[:count], refs[count : 2 * count], refs[2 * count : 2 * count + added]
    width = tables[0].shape[1]
    scale = SCALE / math.sqrt(width)
    step = min(width, 256)
    held = slice(part * LANES, (part + 1) * LANES)
    for k, out in enumerate(refs[-count:]):
        for c in range(0, width, step):
            columns = slice(c, c + step)
            mixed = jnp.dot(state[...], tables[k][:, columns], preferred_element_type=jnp.float32)
            kept = jnp.where(masks[k][held, columns].astype(jnp.float32) > 0, mixed, 0.0)
            total = jnp.sum(kept, 0, keepdims=True) * scale
            total = total * coords[weights[k] : weights[k] + 1, columns]
            if added:
                total = total + sums[k][:, columns]
            out[:, columns] = total


def last(part, which, state, coords, tables, masks, sums, *after):
    width = state.shape[1]
    count = len(which)
    base = 8 * (LEVELS - 1)
    weights = [base + (WEIGHT, OTHER_WEIGHT)[k] for k in which]
    tables, masks = [tables[k] for k in which], [masks[k] for k in which]
    shape = jax.ShapeDtypeStruct((1, width), jnp.float32)
    return pl.pallas_call(
        functools.partial(last_kernel, part, weights, len(sums)),
        out_shape=(shape,) * count,
        in_specs=[VMEM] * (2 + 2 * count + len(sums)) + [ANY] * len(after),
        out_specs=(VMEM,) * count,
        compiler_params=params(7),
        cost_estimate=cost(24 * count * width * width * 8, 2 * count * width * width),
    )(state, coords, *tables, *masks, *sums, *after)


def on_device(wavefield, redatum_taps, cell_x, cell_depth, slowness, illumination, aperture):
    index = lax.axis_index("space")
    blocks = lax.axis_size("space") // BOXES
    block_bits = blocks.bit_length() - 1
    block = index % blocks
    count, width = wavefield.shape
    depth = cell_depth.reshape(BOXES * width // LANES, LANES)
    light = illumination.reshape(BOXES * width // LANES, LANES)
    near_edge, far_edge, coords = prepare(blocks, wavefield, cell_x, depth, light, slowness)
    mask = mark(aperture)
    near_edge = partner(near_edge, "space", block_bits)
    far_edge = across(far_edge, "space", blocks)
    taps = redatum_taps
    if blocks > 1:
        taps = lax.dynamic_slice_in_dim(redatum_taps, block * count, count, 0)
    taps = taps.T
    parts = range(count // LANES)

    (near,) = tables(0, (0,), coords, mask)
    near_edge, far_edge, held_mask = lax.optimization_barrier((near_edge, far_edge, mask))
    masks = partner(held_mask, "space", LEVELS - 1 + block_bits)
    state = redatum(blocks, near_edge, wavefield, far_edge, taps, near)
    received = partner(state, "space", block_bits)
    (far,) = tables(0, (1,), coords, state)
    states = [state for _ in parts]
    theirs = [received for _ in parts]
    table, ahead = (near, far), far
    both, sums = (mask, masks), ()
    for level in range(LEVELS - 1):
        for part in parts:
            states[part] = mix(part, states[part], theirs[part], *table, ahead)
            ahead = states[part]
            if level + 2 == LEVELS and part + 1 < len(parts):
                sums = last(part, (0, 1), states[part], coords, later, both, sums)
                ahead = sums[0]
            if level + 2 == LEVELS and part + 1 == len(parts):
                final = (states[part], coords, later, both)
                (other,) = last(part, (1,), *final, sums[1:])
                (own,) = last(part, (0,), *final, sums[:1], other)
            if level + 2 < LEVELS:
                theirs[part] = partner(states[part], "space", level + 1 + block_bits)
            if part == (0 if level == 1 else len(parts) - 1) and level < 2:
                following = tables(level + 1, (0, 1), coords, ahead)
                ahead = following[0]
            if part == len(parts) - 1 and level == 1:
                later = tables(level + 2, (0, 1), coords, ahead)
                ahead = later[0]
        table = following
    image = own + partner(other, "space", LEVELS - 1 + block_bits)
    for level in range(block_bits):
        image = image + partner(image, "space", level)
    share = width // blocks
    return lax.dynamic_slice_in_dim(image, block * share, share, 1)


def solution(mesh):
    placed = (
        P(("groups", "space"), None),
        P("groups", None),
        P(),
        P(),
        P(),
        P("groups"),
        P(("groups", "space"), None),
    )
    return jax.shard_map(
        on_device,
        mesh=mesh,
        in_specs=placed,
        out_specs=P(("groups", "space"), None),
        check_vma=False,
    )
```

```python
import functools
import math

import jax
import jax.numpy as jnp
from jax import lax
from jax.experimental import pallas as pl
from jax.experimental.pallas import tpu as pltpu
from jax.sharding import PartitionSpec as P


LEVELS = 4
BOXES = 16
LANES = 128

POLY_A = -0.55846636
POLY_B = 0.08535978
SCALE = -73.58594804
VMEM = pl.BlockSpec(memory_space=pltpu.VMEM)
GRANT = 56 << 20
ANY = pl.BlockSpec(memory_space=pl.ANY)
HBM = pl.BlockSpec(memory_space=pltpu.HBM)
SMEM = pl.BlockSpec(memory_space=pltpu.SMEM)


def params(mib):
    return pltpu.CompilerParams(vmem_limit_bytes=mib << 20)


def cost(flops, moved, transcendentals=0):
    return pl.CostEstimate(flops=flops, bytes_accessed=moved, transcendentals=transcendentals)


def across(shard, axis, blocks):
    devices = lax.axis_size(axis)
    shift = [blocks if i // blocks % 2 else -blocks for i in range(devices)]
    pairs = [(i, i + by) for i, by in enumerate(shift) if 0 <= i + by < devices]
    return lax.ppermute(shard, axis, pairs)


def partner(shard, axis, bit):
    return lax.ppermute(shard, axis, [(i, i ^ 1 << bit) for i in range(lax.axis_size(axis))])


def cosine(squared):
    u = squared * lax.rsqrt(squared)
    r = u - jnp.round(u)
    w = jnp.abs(r) - 0.25
    q = w * w
    return w * ((q + POLY_A) * q + POLY_B)


def boxes_of(level, blocks):
    box = lax.axis_index("space") // blocks
    bit = 1 << level
    upper = (box // bit) % 2
    return box, box + bit - 2 * bit * upper


ROW, OTHER_ROW, COLUMN, BELOW, OTHER_COLUMN, OTHER_BELOW, WEIGHT, OTHER_WEIGHT = range(8)


def prepare_kernel(blocks, count, width, cell_x, depth, illumination, slowness, *refs):
    coords, cells, depths, lights, slow, sems = refs[-6:]
    tall = width // LANES
    box = boxes_of(0, blocks)[0]
    others = [boxes_of(level, blocks)[1] for level in range(LEVELS)]
    copies = [pltpu.make_async_copy(slowness, slow, sems.at[0])]
    for k, which in enumerate([box] + others):
        at = pl.ds(pl.multiple_of(which * width, width), width)
        copies.append(pltpu.make_async_copy(cell_x.at[:, at], cells.at[k], sems.at[1 + k]))
    for k, which in enumerate((box, others[-1])):
        at = pl.ds(pl.multiple_of(which * tall, tall), tall)
        copies.append(pltpu.make_async_copy(depth.at[at, :], depths.at[k], sems.at[6 + k]))
        light = illumination.at[at, :]
        copies.append(pltpu.make_async_copy(light, lights.at[k], sems.at[10 + k]))
    for copy in copies:
        copy.start()
    for copy in copies:
        copy.wait()
    coords[...] = jnp.zeros_like(coords)
    for level in range(LEVELS):
        turns = slow[level] * (0.5 / math.pi)
        base = 8 * level

        def put(kind, source, row):
            coords[base + kind : base + kind + 1, :] = (
                cells[source, row : row + 1, :].astype(jnp.float32) * turns
            )

        def put_below(kind, source):
            for k in range(tall):
                part = depths[source, k : k + 1, :].astype(jnp.float32) * turns
                coords[base + kind : base + kind + 1, k * LANES : (k + 1) * LANES] = part * part

        put(ROW, 0, level)
        put(OTHER_ROW, 1 + level, level)
        put(COLUMN, 0, level + 1)
        put_below(BELOW, 0)
        if level + 1 == LEVELS:
            put(OTHER_COLUMN, LEVELS, level + 1)
            put_below(OTHER_BELOW, 1)
    share = 1.0 / math.sqrt(count * blocks)
    base = 8 * (LEVELS - 1)
    for source, kind in enumerate((WEIGHT, OTHER_WEIGHT)):
        for k in range(tall):
            coords[base + kind : base + kind + 1, k * LANES : (k + 1) * LANES] = (
                lights[source, k : k + 1, :] * share
            )


def mark_kernel(aperture, *refs):
    mask = refs[-1]
    mask[...] = (aperture[...] > 0).astype(jnp.float32).astype(jnp.bfloat16)


def mark(aperture, *after):
    return pl.pallas_call(
        mark_kernel,
        out_shape=jax.ShapeDtypeStruct(aperture.shape, jnp.bfloat16),
        in_specs=[VMEM] + [ANY] * len(after),
        out_specs=VMEM,
        compiler_params=params(4),
        cost_estimate=cost(aperture.size * 200, aperture.size * 6),
        name="mark",
    )(aperture, *after)


def prepare(blocks, count, width, cell_x, depth, illumination, slowness, *after):
    levels = cell_x.shape[0]
    return pl.pallas_call(
        functools.partial(prepare_kernel, blocks, count, width),
        out_shape=jax.ShapeDtypeStruct((8 * LEVELS, width), jnp.float32),
        in_specs=[HBM] * 4 + [ANY] * len(after),
        out_specs=VMEM,
        scratch_shapes=[
            pltpu.VMEM((1 + LEVELS, levels, width), jnp.int32),
            pltpu.VMEM((2, width // LANES, LANES), jnp.int32),
            pltpu.VMEM((2, width // LANES, LANES), jnp.float32),
            pltpu.SMEM((LEVELS,), jnp.float32),
            pltpu.SemaphoreType.DMA((12,)),
        ],
        compiler_params=pltpu.CompilerParams(vmem_limit_bytes=GRANT),
        cost_estimate=cost(24 * 2 * width * width * 15, count * width * 8),
        name="prepare",
    )(cell_x, depth, illumination, slowness, *after)


def tables_kernel(jobs, step, coords, *refs):
    outs, rows = refs[-1 - len(jobs) : -1], refs[-1]
    width = outs[0].shape[0]
    steps = width // step

    def fill(slot, row, i):
        at = pl.ds(pl.multiple_of(i * step, step), step)
        rows[slot] = jnp.broadcast_to(coords[row : row + 1, at], (LANES, step)).T

    for (row, column, below), out in zip(jobs, outs):
        fill(0, row, 0)

        @pl.loop(0, steps)
        def _(i):
            at = pl.ds(pl.multiple_of(i * step, step), step)
            part = rows[i % 2]
            part = jnp.concatenate([part, part], 1)
            for c in range(0, width, 2 * LANES):
                columns = slice(c, c + 2 * LANES)
                across = part - coords[column : column + 1, columns]
                squared = across * across + coords[below : below + 1, columns]
                out[at, columns] = cosine(squared).astype(jnp.bfloat16)
            fill((i + 1) % 2, row, jnp.minimum(i + 1, steps - 1))


def tables(level, which, coords, *after):
    width = coords.shape[1]
    base = 8 * level
    near = (base + ROW, base + COLUMN, base + BELOW)
    far = (base + OTHER_ROW, base + COLUMN, base + BELOW)
    if level + 1 == LEVELS:
        far = (base + ROW, base + OTHER_COLUMN, base + OTHER_BELOW)
    jobs = [(near, far)[k] for k in which]
    shape = jax.ShapeDtypeStruct((width, width), jnp.bfloat16)
    step = LANES
    return pl.pallas_call(
        functools.partial(tables_kernel, jobs, step),
        out_shape=(shape,) * len(jobs),
        in_specs=[VMEM] + [ANY] * len(after),
        out_specs=(VMEM,) * len(jobs),
        scratch_shapes=[pltpu.VMEM((2, step, LANES), jnp.float32)],
        compiler_params=params(6),
        cost_estimate=cost(24 * len(jobs) * width * width * 40, 2 * len(jobs) * width * width),
    )(coords, *after)


def redatum_kernel(reach, blocks, near_edge, wave, far_edge, taps, *refs):
    out, padded = refs[-2:]
    count, width = wave.shape
    edge = near_edge.shape[1]
    even = 1 - boxes_of(0, blocks)[0] % 2
    after = edge + width
    starts = (pl.multiple_of(even * after, LANES), pl.multiple_of((1 - even) * after, LANES))
    for lane in range(count // LANES):
        held = slice(lane * LANES, (lane + 1) * LANES)
        for source, start in ((near_edge, starts[0]), (far_edge, starts[1]), (wave, edge)):
            for x in range(0, source.shape[1], LANES):
                block = source[held, x : x + LANES].astype(jnp.float32)
                padded[lane, pl.ds(start + x, LANES), :] = block.T

        @pl.loop(0, width // LANES)
        def _(block):
            base = pl.multiple_of(block * LANES, LANES)
            total = None
            for j in range(taps.shape[0]):
                weight = jnp.broadcast_to(taps[j : j + 1, held], (LANES, LANES))
                term = weight * padded[lane, pl.ds(base + edge - reach + j, LANES), :]
                total = term if total is None else total + term
            out[held, pl.ds(base, LANES)] = total.T.astype(out.dtype)


def redatum(blocks, near_edge, wave, far_edge, taps, *after):
    count, width = wave.shape
    reach = (taps.shape[0] - 1) // 2
    long = width + 2 * near_edge.shape[1]
    return pl.pallas_call(
        functools.partial(redatum_kernel, reach, blocks),
        out_shape=jax.ShapeDtypeStruct((count, width), jnp.bfloat16),
        in_specs=[VMEM] * 4 + [ANY] * len(after),
        out_specs=VMEM,
        scratch_shapes=[pltpu.VMEM((count // LANES, long, LANES), jnp.float32)],
        compiler_params=params(6),
        cost_estimate=cost(24 * 2 * width * width * 60, count * width * 4),
        name="redatum",
    )(near_edge, wave, far_edge, taps, *after)


def mix_kernel(held, mine, theirs, near, far, *refs):
    out = refs[-1]
    width = near.shape[1]
    scale = SCALE / math.sqrt(width)
    step = min(width, 256)
    for c in range(0, width, step):
        columns = slice(c, c + step)
        total = jnp.dot(mine[held, :], near[:, columns], preferred_element_type=jnp.float32)
        total += jnp.dot(theirs[held, :], far[:, columns], preferred_element_type=jnp.float32)
        out[:, columns] = (total * scale).astype(out.dtype)


def mix(part, mine, theirs, near, far, *after):
    count, width = mine.shape
    held = slice(part * LANES, (part + 1) * LANES) if count > LANES else slice(0, LANES)
    return pl.pallas_call(
        functools.partial(mix_kernel, held),
        out_shape=jax.ShapeDtypeStruct((LANES, width), jnp.bfloat16),
        in_specs=[VMEM] * 4 + [ANY] * len(after),
        out_specs=VMEM,
        compiler_params=params(7),
        cost_estimate=cost(24 * width * width * 15, 4 * width * width),
        name="mix",
    )(mine, theirs, near, far, *after)


def last_kernel(part, weights, added, state, coords, *refs):
    count = len(weights)
    tables, masks, sums = refs[:count], refs[count : 2 * count], refs[2 * count : 2 * count + added]
    width = tables[0].shape[1]
    scale = SCALE / math.sqrt(width)
    step = min(width, 256)
    held = slice(part * LANES, (part + 1) * LANES)
    for k, out in enumerate(refs[-count:]):
        for c in range(0, width, step):
            columns = slice(c, c + step)
            mixed = jnp.dot(state[...], tables[k][:, columns], preferred_element_type=jnp.float32)
            kept = jnp.where(masks[k][held, columns].astype(jnp.float32) > 0, mixed, 0.0)
            total = jnp.sum(kept, 0, keepdims=True) * scale
            total = total * coords[weights[k] : weights[k] + 1, columns]
            if added:
                total = total + sums[k][:, columns]
            out[:, columns] = total


def last(part, which, state, coords, tables, masks, sums, *after):
    width = state.shape[1]
    count = len(which)
    base = 8 * (LEVELS - 1)
    weights = [base + (WEIGHT, OTHER_WEIGHT)[k] for k in which]
    tables, masks = [tables[k] for k in which], [masks[k] for k in which]
    shape = jax.ShapeDtypeStruct((1, width), jnp.float32)
    return pl.pallas_call(
        functools.partial(last_kernel, part, weights, len(sums)),
        out_shape=(shape,) * count,
        in_specs=[VMEM] * (2 + 2 * count + len(sums)) + [ANY] * len(after),
        out_specs=(VMEM,) * count,
        compiler_params=params(7),
        cost_estimate=cost(24 * count * width * width * 8, 2 * count * width * width),
    )(state, coords, *tables, *masks, *sums, *after)


def on_device(wavefield, redatum_taps, cell_x, cell_depth, slowness, illumination, aperture):
    index = lax.axis_index("space")
    blocks = lax.axis_size("space") // BOXES
    block_bits = blocks.bit_length() - 1
    block = index % blocks
    count, width = wavefield.shape
    depth = cell_depth.reshape(BOXES * width // LANES, LANES)
    light = illumination.reshape(BOXES * width // LANES, LANES)
    even = index // blocks % 2 == 0
    head, tail = wavefield[:, :LANES], wavefield[:, width - LANES :]
    far_edge = across(jnp.where(even, head, tail), "space", blocks)
    near_edge = partner(jnp.where(even, tail, head), "space", block_bits)
    coords = prepare(blocks, count, width, cell_x, depth, light, slowness)
    mask = mark(aperture)
    taps = redatum_taps
    if blocks > 1:
        taps = lax.dynamic_slice_in_dim(redatum_taps, block * count, count, 0)
    taps = taps.T
    parts = range(count // LANES)

    near_edge, far_edge, held_mask = lax.optimization_barrier((near_edge, far_edge, mask))
    masks = partner(held_mask, "space", LEVELS - 1 + block_bits)
    (near,) = tables(0, (0,), coords, near_edge)
    state = redatum(blocks, near_edge, wavefield, far_edge, taps, near)
    received = partner(state, "space", block_bits)
    (far,) = tables(0, (1,), coords, state)
    states = [state for _ in parts]
    theirs = [received for _ in parts]
    table, ahead = (near, far), far
    both, sums = (mask, masks), ()
    for level in range(LEVELS - 1):
        for part in parts:
            states[part] = mix(part, states[part], theirs[part], *table, ahead)
            ahead = states[part]
            if level + 2 == LEVELS and part + 1 < len(parts):
                sums = last(part, (0, 1), states[part], coords, later, both, sums)
                ahead = sums[0]
            if level + 2 == LEVELS and part + 1 == len(parts):
                final = (states[part], coords, later, both)
                (other,) = last(part, (1,), *final, sums[1:])
                (own,) = last(part, (0,), *final, sums[:1], other)
            if level + 2 < LEVELS:
                theirs[part] = partner(states[part], "space", level + 1 + block_bits)
            if part == (0 if level == 1 else len(parts) - 1) and level < 2:
                following = tables(level + 1, (0, 1), coords, ahead)
                ahead = following[0]
            if part == len(parts) - 1 and level == 1:
                later = tables(level + 2, (0, 1), coords, ahead)
                ahead = later[0]
        table = following
    image = own + partner(other, "space", LEVELS - 1 + block_bits)
    for level in range(block_bits):
        image = image + partner(image, "space", level)
    share = width // blocks
    return lax.dynamic_slice_in_dim(image, block * share, share, 1)


def solution(mesh):
    placed = (
        P(("groups", "space"), None),
        P("groups", None),
        P(),
        P(),
        P(),
        P("groups"),
        P(("groups", "space"), None),
    )
    return jax.shard_map(
        on_device,
        mesh=mesh,
        in_specs=placed,
        out_specs=P(("groups", "space"), None),
        check_vma=False,
    )
```

```python
import functools
import math

import jax
import jax.numpy as jnp
from jax import lax
from jax.experimental import pallas as pl
from jax.experimental.pallas import tpu as pltpu
from jax.sharding import PartitionSpec as P


LEVELS = 4
BOXES = 16
LANES = 128

POLY_A = -0.55846636
POLY_B = 0.08535978
SCALE = -73.58594804
VMEM = pl.BlockSpec(memory_space=pltpu.VMEM)
GRANT = 56 << 20
ANY = pl.BlockSpec(memory_space=pl.ANY)
HBM = pl.BlockSpec(memory_space=pltpu.HBM)
SMEM = pl.BlockSpec(memory_space=pltpu.SMEM)


def params(mib):
    return pltpu.CompilerParams(vmem_limit_bytes=mib << 20)


def cost(flops, moved, transcendentals=0):
    return pl.CostEstimate(flops=flops, bytes_accessed=moved, transcendentals=transcendentals)


def across(shard, axis, blocks):
    devices = lax.axis_size(axis)
    shift = [blocks if i // blocks % 2 else -blocks for i in range(devices)]
    pairs = [(i, i + by) for i, by in enumerate(shift) if 0 <= i + by < devices]
    return lax.ppermute(shard, axis, pairs)


def partner(shard, axis, bit):
    return lax.ppermute(shard, axis, [(i, i ^ 1 << bit) for i in range(lax.axis_size(axis))])


def cosine(squared):
    u = squared * lax.rsqrt(squared)
    r = u - jnp.round(u)
    w = jnp.abs(r) - 0.25
    q = w * w
    return w * ((q + POLY_A) * q + POLY_B)


def boxes_of(level, blocks):
    box = lax.axis_index("space") // blocks
    bit = 1 << level
    upper = (box // bit) % 2
    return box, box + bit - 2 * bit * upper


ROW, OTHER_ROW, COLUMN, BELOW, OTHER_COLUMN, OTHER_BELOW, WEIGHT, OTHER_WEIGHT = range(8)


def prepare_kernel(blocks, count, width, aperture, cell_x, depth, illumination, slowness, *refs):
    mask, coords, cells, depths, lights, slow, marks, sems = refs[-8:]
    tall = width // LANES
    box = boxes_of(0, blocks)[0]
    others = [boxes_of(level, blocks)[1] for level in range(LEVELS)]
    copies = [pltpu.make_async_copy(slowness, slow, sems.at[0])]
    for k, which in enumerate([box] + others):
        at = pl.ds(pl.multiple_of(which * width, width), width)
        copies.append(pltpu.make_async_copy(cell_x.at[:, at], cells.at[k], sems.at[1 + k]))
    for k, which in enumerate((box, others[-1])):
        at = pl.ds(pl.multiple_of(which * tall, tall), tall)
        copies.append(pltpu.make_async_copy(depth.at[at, :], depths.at[k], sems.at[6 + k]))
        light = illumination.at[at, :]
        copies.append(pltpu.make_async_copy(light, lights.at[k], sems.at[10 + k]))
    marking = pltpu.make_async_copy(aperture, marks, sems.at[8])
    for copy in copies + [marking]:
        copy.start()
    for copy in copies:
        copy.wait()
    coords[...] = jnp.zeros_like(coords)
    for level in range(LEVELS):
        turns = slow[level] * (0.5 / math.pi)
        base = 8 * level

        def put(kind, source, row):
            coords[base + kind : base + kind + 1, :] = (
                cells[source, row : row + 1, :].astype(jnp.float32) * turns
            )

        def put_below(kind, source):
            for k in range(tall):
                part = depths[source, k : k + 1, :].astype(jnp.float32) * turns
                coords[base + kind : base + kind + 1, k * LANES : (k + 1) * LANES] = part * part

        put(ROW, 0, level)
        put(OTHER_ROW, 1 + level, level)
        put(COLUMN, 0, level + 1)
        put_below(BELOW, 0)
        if level + 1 == LEVELS:
            put(OTHER_COLUMN, LEVELS, level + 1)
            put_below(OTHER_BELOW, 1)
    share = 1.0 / math.sqrt(count * blocks)
    base = 8 * (LEVELS - 1)
    for source, kind in enumerate((WEIGHT, OTHER_WEIGHT)):
        for k in range(tall):
            coords[base + kind : base + kind + 1, k * LANES : (k + 1) * LANES] = (
                lights[source, k : k + 1, :] * share
            )
    marking.wait()
    mask[...] = (marks[...] > 0).astype(jnp.float32).astype(jnp.bfloat16)


def prepare(blocks, aperture, cell_x, depth, illumination, slowness):
    count, width = aperture.shape
    levels = cell_x.shape[0]
    return pl.pallas_call(
        functools.partial(prepare_kernel, blocks, count, width),
        out_shape=(
            jax.ShapeDtypeStruct((count, width), jnp.bfloat16),
            jax.ShapeDtypeStruct((8 * LEVELS, width), jnp.float32),
        ),
        in_specs=[HBM] * 5,
        out_specs=(VMEM, VMEM),
        scratch_shapes=[
            pltpu.VMEM((1 + LEVELS, levels, width), jnp.int32),
            pltpu.VMEM((2, width // LANES, LANES), jnp.int32),
            pltpu.VMEM((2, width // LANES, LANES), jnp.float32),
            pltpu.SMEM((LEVELS,), jnp.float32),
            pltpu.VMEM((count, width), jnp.int32),
            pltpu.SemaphoreType.DMA((12,)),
        ],
        compiler_params=pltpu.CompilerParams(vmem_limit_bytes=GRANT),
        cost_estimate=cost(24 * 2 * width * width * 15, count * width * 8),
        name="prepare",
    )(aperture, cell_x, depth, illumination, slowness)


def tables_kernel(jobs, step, coords, *refs):
    outs, rows = refs[-1 - len(jobs) : -1], refs[-1]
    width = outs[0].shape[0]
    steps = width // step

    def fill(slot, row, i):
        at = pl.ds(pl.multiple_of(i * step, step), step)
        rows[slot] = jnp.broadcast_to(coords[row : row + 1, at], (LANES, step)).T

    for (row, column, below), out in zip(jobs, outs):
        fill(0, row, 0)

        @pl.loop(0, steps)
        def _(i):
            at = pl.ds(pl.multiple_of(i * step, step), step)
            part = rows[i % 2]
            part = jnp.concatenate([part, part], 1)
            for c in range(0, width, 2 * LANES):
                columns = slice(c, c + 2 * LANES)
                across = part - coords[column : column + 1, columns]
                squared = across * across + coords[below : below + 1, columns]
                out[at, columns] = cosine(squared).astype(jnp.bfloat16)
            fill((i + 1) % 2, row, jnp.minimum(i + 1, steps - 1))


def tables(level, which, coords, *after):
    width = coords.shape[1]
    base = 8 * level
    near = (base + ROW, base + COLUMN, base + BELOW)
    far = (base + OTHER_ROW, base + COLUMN, base + BELOW)
    if level + 1 == LEVELS:
        far = (base + ROW, base + OTHER_COLUMN, base + OTHER_BELOW)
    jobs = [(near, far)[k] for k in which]
    shape = jax.ShapeDtypeStruct((width, width), jnp.bfloat16)
    step = LANES
    return pl.pallas_call(
        functools.partial(tables_kernel, jobs, step),
        out_shape=(shape,) * len(jobs),
        in_specs=[VMEM] + [ANY] * len(after),
        out_specs=(VMEM,) * len(jobs),
        scratch_shapes=[pltpu.VMEM((2, step, LANES), jnp.float32)],
        compiler_params=params(6),
        cost_estimate=cost(24 * len(jobs) * width * width * 40, 2 * len(jobs) * width * width),
    )(coords, *after)


def redatum_kernel(reach, blocks, near_edge, wave, far_edge, taps, *refs):
    out, padded = refs[-2:]
    count, width = wave.shape
    edge = near_edge.shape[1]
    even = 1 - boxes_of(0, blocks)[0] % 2
    after = edge + width
    starts = (pl.multiple_of(even * after, LANES), pl.multiple_of((1 - even) * after, LANES))
    for lane in range(count // LANES):
        held = slice(lane * LANES, (lane + 1) * LANES)
        for source, start in ((near_edge, starts[0]), (far_edge, starts[1]), (wave, edge)):
            for x in range(0, source.shape[1], LANES):
                block = source[held, x : x + LANES].astype(jnp.float32)
                padded[lane, pl.ds(start + x, LANES), :] = block.T

        @pl.loop(0, width // LANES)
        def _(block):
            base = pl.multiple_of(block * LANES, LANES)
            total = None
            for j in range(taps.shape[0]):
                weight = jnp.broadcast_to(taps[j : j + 1, held], (LANES, LANES))
                term = weight * padded[lane, pl.ds(base + edge - reach + j, LANES), :]
                total = term if total is None else total + term
            out[held, pl.ds(base, LANES)] = total.T.astype(out.dtype)


def redatum(blocks, near_edge, wave, far_edge, taps, *after):
    count, width = wave.shape
    reach = (taps.shape[0] - 1) // 2
    long = width + 2 * near_edge.shape[1]
    return pl.pallas_call(
        functools.partial(redatum_kernel, reach, blocks),
        out_shape=jax.ShapeDtypeStruct((count, width), jnp.bfloat16),
        in_specs=[VMEM] * 4 + [ANY] * len(after),
        out_specs=VMEM,
        scratch_shapes=[pltpu.VMEM((count // LANES, long, LANES), jnp.float32)],
        compiler_params=params(6),
        cost_estimate=cost(24 * 2 * width * width * 60, count * width * 4),
        name="redatum",
    )(near_edge, wave, far_edge, taps, *after)


def mix_kernel(held, mine, theirs, near, far, *refs):
    out = refs[-1]
    width = near.shape[1]
    scale = SCALE / math.sqrt(width)
    step = min(width, 256)
    for c in range(0, width, step):
        columns = slice(c, c + step)
        total = jnp.dot(mine[held, :], near[:, columns], preferred_element_type=jnp.float32)
        total += jnp.dot(theirs[held, :], far[:, columns], preferred_element_type=jnp.float32)
        out[:, columns] = (total * scale).astype(out.dtype)


def mix(part, mine, theirs, near, far, *after):
    count, width = mine.shape
    held = slice(part * LANES, (part + 1) * LANES) if count > LANES else slice(0, LANES)
    return pl.pallas_call(
        functools.partial(mix_kernel, held),
        out_shape=jax.ShapeDtypeStruct((LANES, width), jnp.bfloat16),
        in_specs=[VMEM] * 4 + [ANY] * len(after),
        out_specs=VMEM,
        compiler_params=params(7),
        cost_estimate=cost(24 * width * width * 15, 4 * width * width),
        name="mix",
    )(mine, theirs, near, far, *after)


def last_kernel(part, weights, added, state, coords, *refs):
    count = len(weights)
    tables, masks, sums = refs[:count], refs[count : 2 * count], refs[2 * count : 2 * count + added]
    width = tables[0].shape[1]
    scale = SCALE / math.sqrt(width)
    step = min(width, 256)
    held = slice(part * LANES, (part + 1) * LANES)
    for k, out in enumerate(refs[-count:]):
        for c in range(0, width, step):
            columns = slice(c, c + step)
            mixed = jnp.dot(state[...], tables[k][:, columns], preferred_element_type=jnp.float32)
            kept = jnp.where(masks[k][held, columns].astype(jnp.float32) > 0, mixed, 0.0)
            total = jnp.sum(kept, 0, keepdims=True) * scale
            total = total * coords[weights[k] : weights[k] + 1, columns]
            if added:
                total = total + sums[k][:, columns]
            out[:, columns] = total


def last(part, which, state, coords, tables, masks, sums, *after):
    width = state.shape[1]
    count = len(which)
    base = 8 * (LEVELS - 1)
    weights = [base + (WEIGHT, OTHER_WEIGHT)[k] for k in which]
    tables, masks = [tables[k] for k in which], [masks[k] for k in which]
    shape = jax.ShapeDtypeStruct((1, width), jnp.float32)
    return pl.pallas_call(
        functools.partial(last_kernel, part, weights, len(sums)),
        out_shape=(shape,) * count,
        in_specs=[VMEM] * (2 + 2 * count + len(sums)) + [ANY] * len(after),
        out_specs=(VMEM,) * count,
        compiler_params=params(7),
        cost_estimate=cost(24 * count * width * width * 8, 2 * count * width * width),
    )(state, coords, *tables, *masks, *sums, *after)


def on_device(wavefield, redatum_taps, cell_x, cell_depth, slowness, illumination, aperture):
    index = lax.axis_index("space")
    blocks = lax.axis_size("space") // BOXES
    block_bits = blocks.bit_length() - 1
    block = index % blocks
    count, width = wavefield.shape
    depth = cell_depth.reshape(BOXES * width // LANES, LANES)
    light = illumination.reshape(BOXES * width // LANES, LANES)
    even = index // blocks % 2 == 0
    head, tail = wavefield[:, :LANES], wavefield[:, width - LANES :]
    far_edge = across(jnp.where(even, head, tail), "space", blocks)
    near_edge = partner(jnp.where(even, tail, head), "space", block_bits)
    mask, coords = prepare(blocks, aperture, cell_x, depth, light, slowness)
    taps = redatum_taps
    if blocks > 1:
        taps = lax.dynamic_slice_in_dim(redatum_taps, block * count, count, 0)
    taps = taps.T
    parts = range(count // LANES)

    near_edge, far_edge, held_mask = lax.optimization_barrier((near_edge, far_edge, mask))
    masks = partner(held_mask, "space", LEVELS - 1 + block_bits)
    (near,) = tables(0, (0,), coords, near_edge)
    state = redatum(blocks, near_edge, wavefield, far_edge, taps, near)
    received = partner(state, "space", block_bits)
    (far,) = tables(0, (1,), coords, state)
    states = [state for _ in parts]
    theirs = [received for _ in parts]
    table, ahead = (near, far), far
    both, sums = (mask, masks), ()
    end = len(parts) - 1
    for part in parts:
        states[part] = mix(part, states[part], theirs[part], *table, ahead)
        ahead = states[part]
        theirs[part] = partner(states[part], "space", 1 + block_bits)
    second = tables(1, (0, 1), coords, ahead)
    (near,) = tables(2, (0,), coords, second[0])
    ahead = near
    for part in parts:
        states[part] = mix(part, states[part], theirs[part], *second, ahead)
        ahead = states[part]
        theirs[part] = partner(states[part], "space", 2 + block_bits)
        if part == 0:
            (far,) = tables(2, (1,), coords, ahead)
            ahead = far
    later = tables(3, (0, 1), coords, ahead)
    ahead = later[0]
    for part in parts:
        states[part] = mix(part, states[part], theirs[part], near, far, ahead)
        final = (states[part], coords, later, both)
        if part < end:
            sums = last(part, (0, 1), *final, sums)
            ahead = sums[0]
        else:
            (other,) = last(part, (1,), *final, sums[1:])
            (own,) = last(part, (0,), *final, sums[:1], other)
    image = own + partner(other, "space", LEVELS - 1 + block_bits)
    for level in range(block_bits):
        image = image + partner(image, "space", level)
    share = width // blocks
    return lax.dynamic_slice_in_dim(image, block * share, share, 1)


def solution(mesh):
    placed = (
        P(("groups", "space"), None),
        P("groups", None),
        P(),
        P(),
        P(),
        P("groups"),
        P(("groups", "space"), None),
    )
    return jax.shard_map(
        on_device,
        mesh=mesh,
        in_specs=placed,
        out_specs=P(("groups", "space"), None),
        check_vma=False,
    )
```

```python
import functools
import math

import jax
import jax.numpy as jnp
from jax import lax
from jax.experimental import pallas as pl
from jax.experimental.pallas import tpu as pltpu
from jax.sharding import PartitionSpec as P


LEVELS = 4
BOXES = 16
LANES = 128

POLY_A = -0.55846636
POLY_B = 0.08535978
SCALE = -73.58594804
VMEM = pl.BlockSpec(memory_space=pltpu.VMEM)
GRANT = 56 << 20
ANY = pl.BlockSpec(memory_space=pl.ANY)
HBM = pl.BlockSpec(memory_space=pltpu.HBM)
SMEM = pl.BlockSpec(memory_space=pltpu.SMEM)


def params(mib):
    return pltpu.CompilerParams(vmem_limit_bytes=mib << 20)


def cost(flops, moved, transcendentals=0):
    return pl.CostEstimate(flops=flops, bytes_accessed=moved, transcendentals=transcendentals)


def across(shard, axis, blocks):
    devices = lax.axis_size(axis)
    shift = [blocks if i // blocks % 2 else -blocks for i in range(devices)]
    pairs = [(i, i + by) for i, by in enumerate(shift) if 0 <= i + by < devices]
    return lax.ppermute(shard, axis, pairs)


def partner(shard, axis, bit):
    return lax.ppermute(shard, axis, [(i, i ^ 1 << bit) for i in range(lax.axis_size(axis))])


def cosine(squared):
    u = squared * lax.rsqrt(squared)
    r = u - jnp.round(u)
    w = jnp.abs(r) - 0.25
    q = w * w
    return w * ((q + POLY_A) * q + POLY_B)


def boxes_of(level, blocks):
    box = lax.axis_index("space") // blocks
    bit = 1 << level
    upper = (box // bit) % 2
    return box, box + bit - 2 * bit * upper


ROW, OTHER_ROW, COLUMN, BELOW, OTHER_COLUMN, OTHER_BELOW, WEIGHT, OTHER_WEIGHT = range(8)


def prepare_kernel(blocks, count, width, aperture, cell_x, depth, illumination, slowness, *refs):
    mask, coords, cells, depths, lights, slow, marks, sems = refs[-8:]
    tall = width // LANES
    box = boxes_of(0, blocks)[0]
    others = [boxes_of(level, blocks)[1] for level in range(LEVELS)]
    copies = [pltpu.make_async_copy(slowness, slow, sems.at[0])]
    for k, which in enumerate([box] + others):
        at = pl.ds(pl.multiple_of(which * width, width), width)
        copies.append(pltpu.make_async_copy(cell_x.at[:, at], cells.at[k], sems.at[1 + k]))
    for k, which in enumerate((box, others[-1])):
        at = pl.ds(pl.multiple_of(which * tall, tall), tall)
        copies.append(pltpu.make_async_copy(depth.at[at, :], depths.at[k], sems.at[6 + k]))
        light = illumination.at[at, :]
        copies.append(pltpu.make_async_copy(light, lights.at[k], sems.at[10 + k]))
    marking = pltpu.make_async_copy(aperture, marks, sems.at[8])
    for copy in copies + [marking]:
        copy.start()
    for copy in copies:
        copy.wait()
    coords[...] = jnp.zeros_like(coords)
    for level in range(LEVELS):
        turns = slow[level] * (0.5 / math.pi)
        base = 8 * level

        def put(kind, source, row):
            coords[base + kind : base + kind + 1, :] = (
                cells[source, row : row + 1, :].astype(jnp.float32) * turns
            )

        def put_below(kind, source):
            for k in range(tall):
                part = depths[source, k : k + 1, :].astype(jnp.float32) * turns
                coords[base + kind : base + kind + 1, k * LANES : (k + 1) * LANES] = part * part

        put(ROW, 0, level)
        put(OTHER_ROW, 1 + level, level)
        put(COLUMN, 0, level + 1)
        put_below(BELOW, 0)
        if level + 1 == LEVELS:
            put(OTHER_COLUMN, LEVELS, level + 1)
            put_below(OTHER_BELOW, 1)
    share = 1.0 / math.sqrt(count * blocks)
    base = 8 * (LEVELS - 1)
    for source, kind in enumerate((WEIGHT, OTHER_WEIGHT)):
        for k in range(tall):
            coords[base + kind : base + kind + 1, k * LANES : (k + 1) * LANES] = (
                lights[source, k : k + 1, :] * share
            )
    marking.wait()
    mask[...] = (marks[...] > 0).astype(jnp.float32).astype(jnp.bfloat16)


def prepare(blocks, aperture, cell_x, depth, illumination, slowness):
    count, width = aperture.shape
    levels = cell_x.shape[0]
    return pl.pallas_call(
        functools.partial(prepare_kernel, blocks, count, width),
        out_shape=(
            jax.ShapeDtypeStruct((count, width), jnp.bfloat16),
            jax.ShapeDtypeStruct((8 * LEVELS, width), jnp.float32),
        ),
        in_specs=[HBM] * 5,
        out_specs=(VMEM, VMEM),
        scratch_shapes=[
            pltpu.VMEM((1 + LEVELS, levels, width), jnp.int32),
            pltpu.VMEM((2, width // LANES, LANES), jnp.int32),
            pltpu.VMEM((2, width // LANES, LANES), jnp.float32),
            pltpu.SMEM((LEVELS,), jnp.float32),
            pltpu.VMEM((count, width), jnp.int32),
            pltpu.SemaphoreType.DMA((12,)),
        ],
        compiler_params=pltpu.CompilerParams(vmem_limit_bytes=GRANT),
        cost_estimate=cost(24 * 2 * width * width * 15, count * width * 8),
        name="prepare",
    )(aperture, cell_x, depth, illumination, slowness)


def tables_kernel(jobs, step, coords, *refs):
    outs, rows = refs[-1 - len(jobs) : -1], refs[-1]
    width = outs[0].shape[0]
    steps = width // step

    def fill(slot, row, i):
        at = pl.ds(pl.multiple_of(i * step, step), step)
        rows[slot] = jnp.broadcast_to(coords[row : row + 1, at], (LANES, step)).T

    for (row, column, below), out in zip(jobs, outs):
        fill(0, row, 0)

        @pl.loop(0, steps)
        def _(i):
            at = pl.ds(pl.multiple_of(i * step, step), step)
            part = rows[i % 2]
            part = jnp.concatenate([part, part], 1)
            for c in range(0, width, 2 * LANES):
                columns = slice(c, c + 2 * LANES)
                across = part - coords[column : column + 1, columns]
                squared = across * across + coords[below : below + 1, columns]
                out[at, columns] = cosine(squared).astype(jnp.bfloat16)
            fill((i + 1) % 2, row, jnp.minimum(i + 1, steps - 1))


def tables(level, which, coords, *after):
    width = coords.shape[1]
    base = 8 * level
    near = (base + ROW, base + COLUMN, base + BELOW)
    far = (base + OTHER_ROW, base + COLUMN, base + BELOW)
    if level + 1 == LEVELS:
        far = (base + ROW, base + OTHER_COLUMN, base + OTHER_BELOW)
    jobs = [(near, far)[k] for k in which]
    shape = jax.ShapeDtypeStruct((width, width), jnp.bfloat16)
    step = LANES
    return pl.pallas_call(
        functools.partial(tables_kernel, jobs, step),
        out_shape=(shape,) * len(jobs),
        in_specs=[VMEM] + [ANY] * len(after),
        out_specs=(VMEM,) * len(jobs),
        scratch_shapes=[pltpu.VMEM((2, step, LANES), jnp.float32)],
        compiler_params=params(6),
        cost_estimate=cost(24 * len(jobs) * width * width * 40, 2 * len(jobs) * width * width),
    )(coords, *after)


def redatum_kernel(reach, blocks, lane, near_edge, wave, far_edge, taps, *refs):
    out, padded = refs[-2:]
    width = wave.shape[1]
    edge = near_edge.shape[1]
    even = 1 - boxes_of(0, blocks)[0] % 2
    after = edge + width
    starts = (pl.multiple_of(even * after, LANES), pl.multiple_of((1 - even) * after, LANES))
    held = slice(lane * LANES, (lane + 1) * LANES)
    for source, start in ((near_edge, starts[0]), (far_edge, starts[1]), (wave, edge)):
        for x in range(0, source.shape[1], LANES):
            block = source[held, x : x + LANES].astype(jnp.float32)
            padded[pl.ds(start + x, LANES), :] = block.T

    @pl.loop(0, width // LANES)
    def _(block):
        base = pl.multiple_of(block * LANES, LANES)
        total = None
        for j in range(taps.shape[0]):
            weight = jnp.broadcast_to(taps[j : j + 1, held], (LANES, LANES))
            term = weight * padded[pl.ds(base + edge - reach + j, LANES), :]
            total = term if total is None else total + term
        out[:, pl.ds(base, LANES)] = total.T.astype(out.dtype)


def redatum(blocks, part, near_edge, wave, far_edge, taps, *after):
    width = wave.shape[1]
    reach = (taps.shape[0] - 1) // 2
    long = width + 2 * near_edge.shape[1]
    return pl.pallas_call(
        functools.partial(redatum_kernel, reach, blocks, part),
        out_shape=jax.ShapeDtypeStruct((LANES, width), jnp.bfloat16),
        in_specs=[VMEM] * 4 + [ANY] * len(after),
        out_specs=VMEM,
        scratch_shapes=[pltpu.VMEM((long, LANES), jnp.float32)],
        compiler_params=params(6),
        cost_estimate=cost(24 * 2 * width * width * 30, LANES * width * 4),
    )(near_edge, wave, far_edge, taps, *after)


def mix_kernel(mine, theirs, near, far, *refs):
    out = refs[-1]
    width = near.shape[1]
    scale = SCALE / math.sqrt(width)
    step = min(width, 256)
    for c in range(0, width, step):
        columns = slice(c, c + step)
        total = jnp.dot(mine[...], near[:, columns], preferred_element_type=jnp.float32)
        total += jnp.dot(theirs[...], far[:, columns], preferred_element_type=jnp.float32)
        out[:, columns] = (total * scale).astype(out.dtype)


def mix(mine, theirs, near, far, *after):
    count, width = mine.shape
    return pl.pallas_call(
        mix_kernel,
        out_shape=jax.ShapeDtypeStruct((count, width), jnp.bfloat16),
        in_specs=[VMEM] * 4 + [ANY] * len(after),
        out_specs=VMEM,
        compiler_params=params(7),
        cost_estimate=cost(24 * width * width * 15, 4 * width * width),
        name="mix",
    )(mine, theirs, near, far, *after)


def last_kernel(part, weights, added, state, coords, *refs):
    count = len(weights)
    tables, masks, sums = refs[:count], refs[count : 2 * count], refs[2 * count : 2 * count + added]
    width = tables[0].shape[1]
    scale = SCALE / math.sqrt(width)
    step = min(width, 256)
    held = slice(part * LANES, (part + 1) * LANES)
    for k, out in enumerate(refs[-count:]):
        for c in range(0, width, step):
            columns = slice(c, c + step)
            mixed = jnp.dot(state[...], tables[k][:, columns], preferred_element_type=jnp.float32)
            kept = jnp.where(masks[k][held, columns].astype(jnp.float32) > 0, mixed, 0.0)
            total = jnp.sum(kept, 0, keepdims=True) * scale
            total = total * coords[weights[k] : weights[k] + 1, columns]
            if added:
                total = total + sums[k][:, columns]
            out[:, columns] = total


def last(part, which, state, coords, tables, masks, sums, *after):
    width = state.shape[1]
    count = len(which)
    base = 8 * (LEVELS - 1)
    weights = [base + (WEIGHT, OTHER_WEIGHT)[k] for k in which]
    tables, masks = [tables[k] for k in which], [masks[k] for k in which]
    shape = jax.ShapeDtypeStruct((1, width), jnp.float32)
    return pl.pallas_call(
        functools.partial(last_kernel, part, weights, len(sums)),
        out_shape=(shape,) * count,
        in_specs=[VMEM] * (2 + 2 * count + len(sums)) + [ANY] * len(after),
        out_specs=(VMEM,) * count,
        compiler_params=params(7),
        cost_estimate=cost(24 * count * width * width * 8, 2 * count * width * width),
    )(state, coords, *tables, *masks, *sums, *after)


def on_device(wavefield, redatum_taps, cell_x, cell_depth, slowness, illumination, aperture):
    index = lax.axis_index("space")
    blocks = lax.axis_size("space") // BOXES
    block_bits = blocks.bit_length() - 1
    block = index % blocks
    count, width = wavefield.shape
    depth = cell_depth.reshape(BOXES * width // LANES, LANES)
    light = illumination.reshape(BOXES * width // LANES, LANES)
    even = index // blocks % 2 == 0
    head, tail = wavefield[:, :LANES], wavefield[:, width - LANES :]
    far_edge = across(jnp.where(even, head, tail), "space", blocks)
    near_edge = partner(jnp.where(even, tail, head), "space", block_bits)
    mask, coords = prepare(blocks, aperture, cell_x, depth, light, slowness)
    taps = redatum_taps
    if blocks > 1:
        taps = lax.dynamic_slice_in_dim(redatum_taps, block * count, count, 0)
    taps = taps.T
    parts = range(count // LANES)

    near_edge, far_edge, held_mask = lax.optimization_barrier((near_edge, far_edge, mask))
    masks = partner(held_mask, "space", LEVELS - 1 + block_bits)
    (near,) = tables(0, (0,), coords, near_edge)
    both, sums = (mask, masks), ()
    end = len(parts) - 1
    states, theirs, far = [], [], None
    ahead = near
    for part in parts:
        state = redatum(blocks, part, near_edge, wavefield, far_edge, taps, ahead)
        received = partner(state, "space", block_bits)
        ahead = state
        if part == 0:
            (far,) = tables(0, (1,), coords, ahead)
            ahead = far
        states.append(mix(state, received, near, far, ahead))
        ahead = states[part]
        theirs.append(partner(ahead, "space", 1 + block_bits))
    second = tables(1, (0, 1), coords, ahead)
    ahead = second[0]
    third = []
    for part in parts:
        states[part] = mix(states[part], theirs[part], *second, ahead)
        ahead = states[part]
        theirs[part] = partner(ahead, "space", 2 + block_bits)
        if part == 0:
            third += tables(2, (0,), coords, ahead)
            ahead = third[-1]
        if part == end:
            third += tables(2, (1,), coords, ahead)
            ahead = third[-1]
    later = tables(3, (0, 1), coords, ahead)
    ahead = later[0]
    for part in parts:
        states[part] = mix(states[part], theirs[part], *third, ahead)
        final = (states[part], coords, later, both)
        if part < end:
            sums = last(part, (0, 1), *final, sums)
            ahead = sums[0]
        else:
            (other,) = last(part, (1,), *final, sums[1:])
            (own,) = last(part, (0,), *final, sums[:1], other)
    image = own + partner(other, "space", LEVELS - 1 + block_bits)
    for level in range(block_bits):
        image = image + partner(image, "space", level)
    share = width // blocks
    return lax.dynamic_slice_in_dim(image, block * share, share, 1)


def solution(mesh):
    placed = (
        P(("groups", "space"), None),
        P("groups", None),
        P(),
        P(),
        P(),
        P("groups"),
        P(("groups", "space"), None),
    )
    return jax.shard_map(
        on_device,
        mesh=mesh,
        in_specs=placed,
        out_specs=P(("groups", "space"), None),
        check_vma=False,
    )
```

```python
import functools
import math

import jax
import jax.numpy as jnp
from jax import lax
from jax.experimental import pallas as pl
from jax.experimental.pallas import tpu as pltpu
from jax.sharding import PartitionSpec as P


LEVELS = 4
BOXES = 16
LANES = 128

POLY_A = -0.55846636
POLY_B = 0.08535978
SCALE = -73.58594804
VMEM = pl.BlockSpec(memory_space=pltpu.VMEM)
GRANT = 56 << 20
ANY = pl.BlockSpec(memory_space=pl.ANY)
HBM = pl.BlockSpec(memory_space=pltpu.HBM)
SMEM = pl.BlockSpec(memory_space=pltpu.SMEM)


def params(mib):
    return pltpu.CompilerParams(vmem_limit_bytes=mib << 20)


def cost(flops, moved, transcendentals=0):
    return pl.CostEstimate(flops=flops, bytes_accessed=moved, transcendentals=transcendentals)


def across(shard, axis, blocks):
    devices = lax.axis_size(axis)
    shift = [blocks if i // blocks % 2 else -blocks for i in range(devices)]
    pairs = [(i, i + by) for i, by in enumerate(shift) if 0 <= i + by < devices]
    return lax.ppermute(shard, axis, pairs)


def partner(shard, axis, bit):
    return lax.ppermute(shard, axis, [(i, i ^ 1 << bit) for i in range(lax.axis_size(axis))])


def cosine(squared):
    u = squared * lax.rsqrt(squared)
    r = u - jnp.round(u)
    w = jnp.abs(r) - 0.25
    q = w * w
    return w * ((q + POLY_A) * q + POLY_B)


def boxes_of(level, blocks):
    box = lax.axis_index("space") // blocks
    bit = 1 << level
    upper = (box // bit) % 2
    return box, box + bit - 2 * bit * upper


ROW, OTHER_ROW, COLUMN, BELOW, OTHER_COLUMN, OTHER_BELOW, WEIGHT, OTHER_WEIGHT = range(8)


def prepare_kernel(blocks, count, width, aperture, cell_x, depth, illumination, slowness, *refs):
    mask, coords, cells, depths, lights, slow, marks, sems = refs[-8:]
    tall = width // LANES
    box = boxes_of(0, blocks)[0]
    others = [boxes_of(level, blocks)[1] for level in range(LEVELS)]
    copies = [pltpu.make_async_copy(slowness, slow, sems.at[0])]
    for k, which in enumerate([box] + others):
        at = pl.ds(pl.multiple_of(which * width, width), width)
        copies.append(pltpu.make_async_copy(cell_x.at[:, at], cells.at[k], sems.at[1 + k]))
    for k, which in enumerate((box, others[-1])):
        at = pl.ds(pl.multiple_of(which * tall, tall), tall)
        copies.append(pltpu.make_async_copy(depth.at[at, :], depths.at[k], sems.at[6 + k]))
        light = illumination.at[at, :]
        copies.append(pltpu.make_async_copy(light, lights.at[k], sems.at[10 + k]))
    marking = pltpu.make_async_copy(aperture, marks, sems.at[8])
    for copy in copies + [marking]:
        copy.start()
    for copy in copies:
        copy.wait()
    coords[...] = jnp.zeros_like(coords)
    for level in range(LEVELS):
        turns = slow[level] * (0.5 / math.pi)
        base = 8 * level

        def put(kind, source, row):
            coords[base + kind : base + kind + 1, :] = (
                cells[source, row : row + 1, :].astype(jnp.float32) * turns
            )

        def put_below(kind, source):
            for k in range(tall):
                part = depths[source, k : k + 1, :].astype(jnp.float32) * turns
                coords[base + kind : base + kind + 1, k * LANES : (k + 1) * LANES] = part * part

        put(ROW, 0, level)
        put(OTHER_ROW, 1 + level, level)
        put(COLUMN, 0, level + 1)
        put_below(BELOW, 0)
        if level + 1 == LEVELS:
            put(OTHER_COLUMN, LEVELS, level + 1)
            put_below(OTHER_BELOW, 1)
    share = 1.0 / math.sqrt(count * blocks)
    base = 8 * (LEVELS - 1)
    for source, kind in enumerate((WEIGHT, OTHER_WEIGHT)):
        for k in range(tall):
            coords[base + kind : base + kind + 1, k * LANES : (k + 1) * LANES] = (
                lights[source, k : k + 1, :] * share
            )
    marking.wait()
    mask[...] = (marks[...] > 0).astype(jnp.float32).astype(jnp.bfloat16)


def prepare(blocks, aperture, cell_x, depth, illumination, slowness):
    count, width = aperture.shape
    levels = cell_x.shape[0]
    return pl.pallas_call(
        functools.partial(prepare_kernel, blocks, count, width),
        out_shape=(
            jax.ShapeDtypeStruct((count, width), jnp.bfloat16),
            jax.ShapeDtypeStruct((8 * LEVELS, width), jnp.float32),
        ),
        in_specs=[HBM] * 5,
        out_specs=(VMEM, VMEM),
        scratch_shapes=[
            pltpu.VMEM((1 + LEVELS, levels, width), jnp.int32),
            pltpu.VMEM((2, width // LANES, LANES), jnp.int32),
            pltpu.VMEM((2, width // LANES, LANES), jnp.float32),
            pltpu.SMEM((LEVELS,), jnp.float32),
            pltpu.VMEM((count, width), jnp.int32),
            pltpu.SemaphoreType.DMA((12,)),
        ],
        compiler_params=pltpu.CompilerParams(vmem_limit_bytes=GRANT),
        cost_estimate=cost(24 * 2 * width * width * 15, count * width * 8),
        name="prepare",
    )(aperture, cell_x, depth, illumination, slowness)


def tables_kernel(jobs, step, coords, *refs):
    outs, rows = refs[-1 - len(jobs) : -1], refs[-1]
    width = outs[0].shape[0]
    steps = width // step

    def fill(slot, row, i):
        at = pl.ds(pl.multiple_of(i * step, step), step)
        rows[slot] = jnp.broadcast_to(coords[row : row + 1, at], (LANES, step)).T

    for (row, column, below), out in zip(jobs, outs):
        fill(0, row, 0)

        @pl.loop(0, steps)
        def _(i):
            at = pl.ds(pl.multiple_of(i * step, step), step)
            part = rows[i % 2]
            part = jnp.concatenate([part, part], 1)
            for c in range(0, width, 2 * LANES):
                columns = slice(c, c + 2 * LANES)
                across = part - coords[column : column + 1, columns]
                squared = across * across + coords[below : below + 1, columns]
                out[at, columns] = cosine(squared).astype(jnp.bfloat16)
            fill((i + 1) % 2, row, jnp.minimum(i + 1, steps - 1))


def tables(level, which, coords, *after):
    width = coords.shape[1]
    base = 8 * level
    near = (base + ROW, base + COLUMN, base + BELOW)
    far = (base + OTHER_ROW, base + COLUMN, base + BELOW)
    if level + 1 == LEVELS:
        far = (base + ROW, base + OTHER_COLUMN, base + OTHER_BELOW)
    jobs = [(near, far)[k] for k in which]
    shape = jax.ShapeDtypeStruct((width, width), jnp.bfloat16)
    step = LANES
    return pl.pallas_call(
        functools.partial(tables_kernel, jobs, step),
        out_shape=(shape,) * len(jobs),
        in_specs=[VMEM] + [ANY] * len(after),
        out_specs=(VMEM,) * len(jobs),
        scratch_shapes=[pltpu.VMEM((2, step, LANES), jnp.float32)],
        compiler_params=params(6),
        cost_estimate=cost(24 * len(jobs) * width * width * 40, 2 * len(jobs) * width * width),
    )(coords, *after)


def redatum_kernel(reach, blocks, lane, near_edge, wave, far_edge, taps, *refs):
    out, padded = refs[-2:]
    width = wave.shape[1]
    edge = near_edge.shape[1]
    even = 1 - boxes_of(0, blocks)[0] % 2
    after = edge + width
    starts = (pl.multiple_of(even * after, LANES), pl.multiple_of((1 - even) * after, LANES))
    held = slice(lane * LANES, (lane + 1) * LANES)
    for source, start in ((near_edge, starts[0]), (far_edge, starts[1]), (wave, edge)):
        for x in range(0, source.shape[1], LANES):
            block = source[held, x : x + LANES].astype(jnp.float32)
            padded[pl.ds(start + x, LANES), :] = block.T

    @pl.loop(0, width // LANES)
    def _(block):
        base = pl.multiple_of(block * LANES, LANES)
        total = None
        for j in range(taps.shape[0]):
            weight = jnp.broadcast_to(taps[j : j + 1, held], (LANES, LANES))
            term = weight * padded[pl.ds(base + edge - reach + j, LANES), :]
            total = term if total is None else total + term
        out[:, pl.ds(base, LANES)] = total.T.astype(out.dtype)


def redatum(blocks, part, near_edge, wave, far_edge, taps, *after):
    width = wave.shape[1]
    reach = (taps.shape[0] - 1) // 2
    long = width + 2 * near_edge.shape[1]
    return pl.pallas_call(
        functools.partial(redatum_kernel, reach, blocks, part),
        out_shape=jax.ShapeDtypeStruct((LANES, width), jnp.bfloat16),
        in_specs=[VMEM] * 4 + [ANY] * len(after),
        out_specs=VMEM,
        scratch_shapes=[pltpu.VMEM((long, LANES), jnp.float32)],
        compiler_params=params(6),
        cost_estimate=cost(24 * 2 * width * width * 30, LANES * width * 4),
    )(near_edge, wave, far_edge, taps, *after)


def mix_kernel(mine, theirs, near, far, *refs):
    out = refs[-1]
    width = near.shape[1]
    scale = SCALE / math.sqrt(width)
    step = min(width, 256)
    for c in range(0, width, step):
        columns = slice(c, c + step)
        total = jnp.dot(mine[...], near[:, columns], preferred_element_type=jnp.float32)
        total += jnp.dot(theirs[...], far[:, columns], preferred_element_type=jnp.float32)
        out[:, columns] = (total * scale).astype(out.dtype)


def mix(mine, theirs, near, far, *after):
    count, width = mine.shape
    return pl.pallas_call(
        mix_kernel,
        out_shape=jax.ShapeDtypeStruct((count, width), jnp.bfloat16),
        in_specs=[VMEM] * 4 + [ANY] * len(after),
        out_specs=VMEM,
        compiler_params=params(7),
        cost_estimate=cost(24 * width * width * 15, 4 * width * width),
        name="mix",
    )(mine, theirs, near, far, *after)


def last_kernel(part, weights, added, state, coords, *refs):
    count = len(weights)
    tables, masks, sums = refs[:count], refs[count : 2 * count], refs[2 * count : 2 * count + added]
    width = tables[0].shape[1]
    scale = SCALE / math.sqrt(width)
    step = min(width, 256)
    held = slice(part * LANES, (part + 1) * LANES)
    for k, out in enumerate(refs[-count:]):
        for c in range(0, width, step):
            columns = slice(c, c + step)
            mixed = jnp.dot(state[...], tables[k][:, columns], preferred_element_type=jnp.float32)
            kept = jnp.where(masks[k][held, columns].astype(jnp.float32) > 0, mixed, 0.0)
            total = jnp.sum(kept, 0, keepdims=True) * scale
            total = total * coords[weights[k] : weights[k] + 1, columns]
            if added:
                total = total + sums[k][:, columns]
            out[:, columns] = total


def last(part, which, state, coords, tables, masks, sums, *after):
    width = state.shape[1]
    count = len(which)
    base = 8 * (LEVELS - 1)
    weights = [base + (WEIGHT, OTHER_WEIGHT)[k] for k in which]
    tables, masks = [tables[k] for k in which], [masks[k] for k in which]
    shape = jax.ShapeDtypeStruct((1, width), jnp.float32)
    return pl.pallas_call(
        functools.partial(last_kernel, part, weights, len(sums)),
        out_shape=(shape,) * count,
        in_specs=[VMEM] * (2 + 2 * count + len(sums)) + [ANY] * len(after),
        out_specs=(VMEM,) * count,
        compiler_params=params(7),
        cost_estimate=cost(24 * count * width * width * 8, 2 * count * width * width),
    )(state, coords, *tables, *masks, *sums, *after)


def on_device(wavefield, redatum_taps, cell_x, cell_depth, slowness, illumination, aperture):
    index = lax.axis_index("space")
    blocks = lax.axis_size("space") // BOXES
    block_bits = blocks.bit_length() - 1
    block = index % blocks
    count, width = wavefield.shape
    depth = cell_depth.reshape(BOXES * width // LANES, LANES)
    light = illumination.reshape(BOXES * width // LANES, LANES)
    even = index // blocks % 2 == 0
    head, tail = wavefield[:, :LANES], wavefield[:, width - LANES :]
    far_edge = across(jnp.where(even, head, tail), "space", blocks)
    near_edge = partner(jnp.where(even, tail, head), "space", block_bits)
    mask, coords = prepare(blocks, aperture, cell_x, depth, light, slowness)
    taps = redatum_taps
    if blocks > 1:
        taps = lax.dynamic_slice_in_dim(redatum_taps, block * count, count, 0)
    taps = taps.T
    parts = range(count // LANES)

    near_edge, far_edge, held_mask = lax.optimization_barrier((near_edge, far_edge, mask))
    masks = partner(held_mask, "space", LEVELS - 1 + block_bits)
    (near,) = tables(0, (0,), coords, near_edge)
    both, sums = (mask, masks), ()
    end = len(parts) - 1
    states, theirs, second, far = [], [], [], None
    ahead = near
    for part in parts:
        state = redatum(blocks, part, near_edge, wavefield, far_edge, taps, ahead)
        received = partner(state, "space", block_bits)
        ahead = state
        if part == 0:
            (far,) = tables(0, (1,), coords, ahead)
            ahead = far
        if part == end:
            second += tables(1, (0,), coords, ahead)
            ahead = second[0]
        states.append(mix(state, received, near, far, ahead))
        ahead = states[part]
        theirs.append(partner(ahead, "space", 1 + block_bits))
    second += tables(1, (1,), coords, ahead)
    ahead = second[-1]
    third = []
    for part in parts:
        states[part] = mix(states[part], theirs[part], *second, ahead)
        ahead = states[part]
        theirs[part] = partner(ahead, "space", 2 + block_bits)
        if part == 0:
            third += tables(2, (0,), coords, ahead)
            ahead = third[-1]
        if part == end:
            third += tables(2, (1,), coords, ahead)
            ahead = third[-1]
    later = tables(3, (0, 1), coords, ahead)
    ahead = later[0]
    for part in parts:
        states[part] = mix(states[part], theirs[part], *third, ahead)
        final = (states[part], coords, later, both)
        if part < end:
            sums = last(part, (0, 1), *final, sums)
            ahead = sums[0]
        else:
            (other,) = last(part, (1,), *final, sums[1:])
            (own,) = last(part, (0,), *final, sums[:1], other)
    image = own + partner(other, "space", LEVELS - 1 + block_bits)
    for level in range(block_bits):
        image = image + partner(image, "space", level)
    share = width // blocks
    return lax.dynamic_slice_in_dim(image, block * share, share, 1)


def solution(mesh):
    placed = (
        P(("groups", "space"), None),
        P("groups", None),
        P(),
        P(),
        P(),
        P("groups"),
        P(("groups", "space"), None),
    )
    return jax.shard_map(
        on_device,
        mesh=mesh,
        in_specs=placed,
        out_specs=P(("groups", "space"), None),
        check_vma=False,
    )
```

```python
import functools
import math

import jax
import jax.numpy as jnp
from jax import lax
from jax.experimental import pallas as pl
from jax.experimental.pallas import tpu as pltpu
from jax.sharding import PartitionSpec as P


LEVELS = 4
BOXES = 16
LANES = 128

POLY_A = -0.55846636
POLY_B = 0.08535978
SCALE = -73.58594804
VMEM = pl.BlockSpec(memory_space=pltpu.VMEM)
GRANT = 56 << 20
ANY = pl.BlockSpec(memory_space=pl.ANY)
HBM = pl.BlockSpec(memory_space=pltpu.HBM)
SMEM = pl.BlockSpec(memory_space=pltpu.SMEM)


def params(mib):
    return pltpu.CompilerParams(vmem_limit_bytes=mib << 20)


def cost(flops, moved, transcendentals=0):
    return pl.CostEstimate(flops=flops, bytes_accessed=moved, transcendentals=transcendentals)


def across(shard, axis, blocks):
    devices = lax.axis_size(axis)
    shift = [blocks if i // blocks % 2 else -blocks for i in range(devices)]
    pairs = [(i, i + by) for i, by in enumerate(shift) if 0 <= i + by < devices]
    return lax.ppermute(shard, axis, pairs)


def partner(shard, axis, bit):
    return lax.ppermute(shard, axis, [(i, i ^ 1 << bit) for i in range(lax.axis_size(axis))])


def cosine(squared):
    u = squared * lax.rsqrt(squared)
    r = u - jnp.round(u)
    w = jnp.abs(r) - 0.25
    q = w * w
    return w * ((q + POLY_A) * q + POLY_B)


def boxes_of(level, blocks):
    box = lax.axis_index("space") // blocks
    bit = 1 << level
    upper = (box // bit) % 2
    return box, box + bit - 2 * bit * upper


ROW, OTHER_ROW, COLUMN, BELOW, OTHER_COLUMN, OTHER_BELOW, WEIGHT, OTHER_WEIGHT = range(8)


def prepare_kernel(blocks, count, width, aperture, cell_x, depth, illumination, slowness, *refs):
    mask, coords, cells, depths, lights, slow, marks, sems = refs[-8:]
    tall = width // LANES
    box = boxes_of(0, blocks)[0]
    others = [boxes_of(level, blocks)[1] for level in range(LEVELS)]
    copies = [pltpu.make_async_copy(slowness, slow, sems.at[0])]
    for k, which in enumerate([box] + others):
        at = pl.ds(pl.multiple_of(which * width, width), width)
        copies.append(pltpu.make_async_copy(cell_x.at[:, at], cells.at[k], sems.at[1 + k]))
    for k, which in enumerate((box, others[-1])):
        at = pl.ds(pl.multiple_of(which * tall, tall), tall)
        copies.append(pltpu.make_async_copy(depth.at[at, :], depths.at[k], sems.at[6 + k]))
        light = illumination.at[at, :]
        copies.append(pltpu.make_async_copy(light, lights.at[k], sems.at[10 + k]))
    marking = pltpu.make_async_copy(aperture, marks, sems.at[8])
    for copy in copies + [marking]:
        copy.start()
    for copy in copies:
        copy.wait()
    coords[...] = jnp.zeros_like(coords)
    for level in range(LEVELS):
        turns = slow[level] * (0.5 / math.pi)
        base = 8 * level

        def put(kind, source, row):
            coords[base + kind : base + kind + 1, :] = (
                cells[source, row : row + 1, :].astype(jnp.float32) * turns
            )

        def put_below(kind, source):
            for k in range(tall):
                part = depths[source, k : k + 1, :].astype(jnp.float32) * turns
                coords[base + kind : base + kind + 1, k * LANES : (k + 1) * LANES] = part * part

        put(ROW, 0, level)
        put(OTHER_ROW, 1 + level, level)
        put(COLUMN, 0, level + 1)
        put_below(BELOW, 0)
        if level + 1 == LEVELS:
            put(OTHER_COLUMN, LEVELS, level + 1)
            put_below(OTHER_BELOW, 1)
    share = 1.0 / math.sqrt(count * blocks)
    base = 8 * (LEVELS - 1)
    for source, kind in enumerate((WEIGHT, OTHER_WEIGHT)):
        for k in range(tall):
            coords[base + kind : base + kind + 1, k * LANES : (k + 1) * LANES] = (
                lights[source, k : k + 1, :] * share
            )
    marking.wait()
    mask[...] = (marks[...] > 0).astype(jnp.float32).astype(jnp.bfloat16)


def prepare(blocks, aperture, cell_x, depth, illumination, slowness):
    count, width = aperture.shape
    levels = cell_x.shape[0]
    return pl.pallas_call(
        functools.partial(prepare_kernel, blocks, count, width),
        out_shape=(
            jax.ShapeDtypeStruct((count, width), jnp.bfloat16),
            jax.ShapeDtypeStruct((8 * LEVELS, width), jnp.float32),
        ),
        in_specs=[HBM] * 5,
        out_specs=(VMEM, VMEM),
        scratch_shapes=[
            pltpu.VMEM((1 + LEVELS, levels, width), jnp.int32),
            pltpu.VMEM((2, width // LANES, LANES), jnp.int32),
            pltpu.VMEM((2, width // LANES, LANES), jnp.float32),
            pltpu.SMEM((LEVELS,), jnp.float32),
            pltpu.VMEM((count, width), jnp.int32),
            pltpu.SemaphoreType.DMA((12,)),
        ],
        compiler_params=pltpu.CompilerParams(vmem_limit_bytes=GRANT),
        cost_estimate=cost(24 * 2 * width * width * 15, count * width * 8),
        name="prepare",
    )(aperture, cell_x, depth, illumination, slowness)


def tables_kernel(jobs, step, coords, *refs):
    outs, rows = refs[-1 - len(jobs) : -1], refs[-1]
    width = outs[0].shape[0]
    steps = width // step

    def fill(slot, row, i):
        at = pl.ds(pl.multiple_of(i * step, step), step)
        rows[slot] = jnp.broadcast_to(coords[row : row + 1, at], (LANES, step)).T

    for (row, column, below), out in zip(jobs, outs):
        fill(0, row, 0)

        @pl.loop(0, steps, unroll=2)
        def _(i):
            at = pl.ds(pl.multiple_of(i * step, step), step)
            part = rows[i % 2]
            part = jnp.concatenate([part, part], 1)
            for c in range(0, width, 2 * LANES):
                columns = slice(c, c + 2 * LANES)
                across = part - coords[column : column + 1, columns]
                squared = across * across + coords[below : below + 1, columns]
                out[at, columns] = cosine(squared).astype(jnp.bfloat16)
            fill((i + 1) % 2, row, jnp.minimum(i + 1, steps - 1))


def tables(level, which, coords, *after):
    width = coords.shape[1]
    base = 8 * level
    near = (base + ROW, base + COLUMN, base + BELOW)
    far = (base + OTHER_ROW, base + COLUMN, base + BELOW)
    if level + 1 == LEVELS:
        far = (base + ROW, base + OTHER_COLUMN, base + OTHER_BELOW)
    jobs = [(near, far)[k] for k in which]
    shape = jax.ShapeDtypeStruct((width, width), jnp.bfloat16)
    step = LANES
    return pl.pallas_call(
        functools.partial(tables_kernel, jobs, step),
        out_shape=(shape,) * len(jobs),
        in_specs=[VMEM] + [ANY] * len(after),
        out_specs=(VMEM,) * len(jobs),
        scratch_shapes=[pltpu.VMEM((2, step, LANES), jnp.float32)],
        compiler_params=params(6),
        cost_estimate=cost(24 * len(jobs) * width * width * 40, 2 * len(jobs) * width * width),
    )(coords, *after)


def redatum_kernel(reach, blocks, lane, near_edge, wave, far_edge, taps, *refs):
    out, padded = refs[-2:]
    width = wave.shape[1]
    edge = near_edge.shape[1]
    even = 1 - boxes_of(0, blocks)[0] % 2
    after = edge + width
    starts = (pl.multiple_of(even * after, LANES), pl.multiple_of((1 - even) * after, LANES))
    held = slice(lane * LANES, (lane + 1) * LANES)
    for source, start in ((near_edge, starts[0]), (far_edge, starts[1]), (wave, edge)):
        for x in range(0, source.shape[1], LANES):
            block = source[held, x : x + LANES].astype(jnp.float32)
            padded[pl.ds(start + x, LANES), :] = block.T

    @pl.loop(0, width // LANES)
    def _(block):
        base = pl.multiple_of(block * LANES, LANES)
        total = None
        for j in range(taps.shape[0]):
            weight = jnp.broadcast_to(taps[j : j + 1, held], (LANES, LANES))
            term = weight * padded[pl.ds(base + edge - reach + j, LANES), :]
            total = term if total is None else total + term
        out[:, pl.ds(base, LANES)] = total.T.astype(out.dtype)


def redatum(blocks, part, near_edge, wave, far_edge, taps, *after):
    width = wave.shape[1]
    reach = (taps.shape[0] - 1) // 2
    long = width + 2 * near_edge.shape[1]
    return pl.pallas_call(
        functools.partial(redatum_kernel, reach, blocks, part),
        out_shape=jax.ShapeDtypeStruct((LANES, width), jnp.bfloat16),
        in_specs=[VMEM] * 4 + [ANY] * len(after),
        out_specs=VMEM,
        scratch_shapes=[pltpu.VMEM((long, LANES), jnp.float32)],
        compiler_params=params(6),
        cost_estimate=cost(24 * 2 * width * width * 30, LANES * width * 4),
    )(near_edge, wave, far_edge, taps, *after)


def mix_kernel(mine, theirs, near, far, *refs):
    out = refs[-1]
    width = near.shape[1]
    scale = SCALE / math.sqrt(width)
    step = min(width, 256)
    for c in range(0, width, step):
        columns = slice(c, c + step)
        total = jnp.dot(mine[...], near[:, columns], preferred_element_type=jnp.float32)
        total += jnp.dot(theirs[...], far[:, columns], preferred_element_type=jnp.float32)
        out[:, columns] = (total * scale).astype(out.dtype)


def mix(mine, theirs, near, far, *after):
    count, width = mine.shape
    return pl.pallas_call(
        mix_kernel,
        out_shape=jax.ShapeDtypeStruct((count, width), jnp.bfloat16),
        in_specs=[VMEM] * 4 + [ANY] * len(after),
        out_specs=VMEM,
        compiler_params=params(7),
        cost_estimate=cost(24 * width * width * 15, 4 * width * width),
        name="mix",
    )(mine, theirs, near, far, *after)


def last_kernel(part, weights, added, state, coords, *refs):
    count = len(weights)
    tables, masks, sums = refs[:count], refs[count : 2 * count], refs[2 * count : 2 * count + added]
    width = tables[0].shape[1]
    scale = SCALE / math.sqrt(width)
    step = min(width, 256)
    held = slice(part * LANES, (part + 1) * LANES)
    for k, out in enumerate(refs[-count:]):
        for c in range(0, width, step):
            columns = slice(c, c + step)
            mixed = jnp.dot(state[...], tables[k][:, columns], preferred_element_type=jnp.float32)
            kept = jnp.where(masks[k][held, columns].astype(jnp.float32) > 0, mixed, 0.0)
            total = jnp.sum(kept, 0, keepdims=True) * scale
            total = total * coords[weights[k] : weights[k] + 1, columns]
            if added:
                total = total + sums[k][:, columns]
            out[:, columns] = total


def last(part, which, state, coords, tables, masks, sums, *after):
    width = state.shape[1]
    count = len(which)
    base = 8 * (LEVELS - 1)
    weights = [base + (WEIGHT, OTHER_WEIGHT)[k] for k in which]
    tables, masks = [tables[k] for k in which], [masks[k] for k in which]
    shape = jax.ShapeDtypeStruct((1, width), jnp.float32)
    return pl.pallas_call(
        functools.partial(last_kernel, part, weights, len(sums)),
        out_shape=(shape,) * count,
        in_specs=[VMEM] * (2 + 2 * count + len(sums)) + [ANY] * len(after),
        out_specs=(VMEM,) * count,
        compiler_params=params(7),
        cost_estimate=cost(24 * count * width * width * 8, 2 * count * width * width),
    )(state, coords, *tables, *masks, *sums, *after)


def on_device(wavefield, redatum_taps, cell_x, cell_depth, slowness, illumination, aperture):
    index = lax.axis_index("space")
    blocks = lax.axis_size("space") // BOXES
    block_bits = blocks.bit_length() - 1
    block = index % blocks
    count, width = wavefield.shape
    depth = cell_depth.reshape(BOXES * width // LANES, LANES)
    light = illumination.reshape(BOXES * width // LANES, LANES)
    even = index // blocks % 2 == 0
    head, tail = wavefield[:, :LANES], wavefield[:, width - LANES :]
    far_edge = across(jnp.where(even, head, tail), "space", blocks)
    near_edge = partner(jnp.where(even, tail, head), "space", block_bits)
    mask, coords = prepare(blocks, aperture, cell_x, depth, light, slowness)
    taps = redatum_taps
    if blocks > 1:
        taps = lax.dynamic_slice_in_dim(redatum_taps, block * count, count, 0)
    taps = taps.T
    parts = range(count // LANES)

    near_edge, far_edge, held_mask = lax.optimization_barrier((near_edge, far_edge, mask))
    masks = partner(held_mask, "space", LEVELS - 1 + block_bits)
    (near,) = tables(0, (0,), coords, near_edge)
    both, sums = (mask, masks), ()
    end = len(parts) - 1
    states, theirs, second, far = [], [], [], None
    ahead = near
    for part in parts:
        state = redatum(blocks, part, near_edge, wavefield, far_edge, taps, ahead)
        received = partner(state, "space", block_bits)
        ahead = state
        if part == 0:
            (far,) = tables(0, (1,), coords, ahead)
            ahead = far
        if part == end:
            second += tables(1, (0,), coords, ahead)
            ahead = second[0]
        states.append(mix(state, received, near, far, ahead))
        ahead = states[part]
        theirs.append(partner(ahead, "space", 1 + block_bits))
    second += tables(1, (1,), coords, ahead)
    ahead = second[-1]
    for part in parts:
        states[part] = mix(states[part], theirs[part], *second, ahead)
        ahead = states[part]
        theirs[part] = partner(ahead, "space", 2 + block_bits)
        if part == 0:
            third = tables(2, (0, 1), coords, ahead)
            ahead = third[0]
    later = tables(3, (0, 1), coords, ahead)
    ahead = later[0]
    for part in parts:
        states[part] = mix(states[part], theirs[part], *third, ahead)
        final = (states[part], coords, later, both)
        if part < end:
            sums = last(part, (0, 1), *final, sums)
            ahead = sums[0]
        else:
            (other,) = last(part, (1,), *final, sums[1:])
            (own,) = last(part, (0,), *final, sums[:1], other)
    image = own + partner(other, "space", LEVELS - 1 + block_bits)
    for level in range(block_bits):
        image = image + partner(image, "space", level)
    share = width // blocks
    return lax.dynamic_slice_in_dim(image, block * share, share, 1)


def solution(mesh):
    placed = (
        P(("groups", "space"), None),
        P("groups", None),
        P(),
        P(),
        P(),
        P("groups"),
        P(("groups", "space"), None),
    )
    return jax.shard_map(
        on_device,
        mesh=mesh,
        in_specs=placed,
        out_specs=P(("groups", "space"), None),
        check_vma=False,
    )
```
